32 devices in a mesh: gx: 4 (over x, core), gy: 4 (over z), gz: 2 (over y).
Axes of the slice: x: 2, y: 2, z: 4, core: 2. Of those that a mesh axis runs over, the one named last changes fastest.
Arguments:
- relative_placements: float32 [3, 12, 12, 8, 128], P(None, 'gx', 'gy', 'gz'), may hold values from 0 to 1
- mass_per_density: float32 [12, 12, 8, 128], P('gx', 'gy', 'gz'), may hold values from 0.004 to 0.04
- opening_heat_level: float32 [12, 12, 8, 128], P('gx', 'gy', 'gz'), may hold values from 0.5 to 2
- bin_fill_counts: int32 [12, 12, 8], P('gx', 'gy', 'gz'), may hold values from 16 to 128
Outputs:
- final_temp: float32 [12, 12, 8, 128], P('gx', 'gy', 'gz')
The draws below stay inside these ranges and needn't reach their ends.
Inputs may be any that keep to these rules, and one draw needn't show every extreme that they name: Tile cell t holds particles in slots 0 to bin_fill_counts[t] - 1; the other slots are empty and are no source.
All inputs are finite; a program needn't handle non-finite values.
Results may differ from the reference program's by a relative error of at most 0.0003.
Values sent between devices are 32-bit elements; how exact they have to be, the bound alone decides.
A program may use at most 64 MiB of HBM per device.

```python
import math
import jax
import jax.numpy as jnp
from jax import lax

BIN_CAPACITY = 128
BLOCK_SPAN_EAST = 12
BLOCK_SPAN_NORTH = 12
BLOCK_SPAN_UPWARD = 8


def with_ends(drawn, own_key, least, largest):
    shape = drawn.shape
    spot = [jax.random.randint(jax.random.fold_in(own_key, axis), (), 0, shape[axis]) for axis in range(len(shape))]
    drawn = drawn.at[tuple(spot)].set(least)
    longest = shape.index(max(shape))
    spot[longest] = (spot[longest] + 1) % shape[longest]
    return drawn.at[tuple(spot)].set(largest)


def levels(rng, extent, split, least, largest):
    factor_of = 1.0
    for dim, shards_of in split:
        draws = jax.random.uniform(jax.random.fold_in(jax.random.fold_in(rng, 6), dim), (shards_of,), jnp.float32, least / len(split), largest / len(split))
        factor_of = factor_of * jnp.repeat(jnp.exp(draws), extent[dim] // shards_of).reshape((-1,) + (1,) * (len(extent) - 1 - dim))
    return factor_of


def setup_inputs(seed: int = 0) -> dict:
    keys = jax.random.split(jax.random.key(seed), 5)
    return {
        "relative_placements": jnp.clip(1.0 * jax.random.uniform(keys[0], (3, BLOCK_SPAN_EAST, BLOCK_SPAN_NORTH, BLOCK_SPAN_UPWARD, BIN_CAPACITY), jnp.float32) ** levels(keys[0], (3, BLOCK_SPAN_EAST, BLOCK_SPAN_NORTH, BLOCK_SPAN_UPWARD, BIN_CAPACITY), ((1, 4), (2, 4), (3, 2)), -0.2, 0.2), 0.0, 1.0),
        "mass_per_density": jnp.clip(jnp.exp(math.log(0.04) - 2.30258502 * jax.random.uniform(keys[1], (BLOCK_SPAN_EAST, BLOCK_SPAN_NORTH, BLOCK_SPAN_UPWARD, BIN_CAPACITY), jnp.float32) ** levels(keys[1], (BLOCK_SPAN_EAST, BLOCK_SPAN_NORTH, BLOCK_SPAN_UPWARD, BIN_CAPACITY), ((0, 4), (1, 4), (2, 2)), -0.2, 0.2)), 0.004, 0.04),
        "opening_heat_level": jnp.clip(jnp.exp(math.log(2.0) - 1.3862944 * jax.random.uniform(keys[2], (BLOCK_SPAN_EAST, BLOCK_SPAN_NORTH, BLOCK_SPAN_UPWARD, BIN_CAPACITY), jnp.float32) ** levels(keys[2], (BLOCK_SPAN_EAST, BLOCK_SPAN_NORTH, BLOCK_SPAN_UPWARD, BIN_CAPACITY), ((0, 4), (1, 4), (2, 2)), -0.2, 0.2)), 0.5, 2.0),
        "bin_fill_counts": with_ends(jax.random.randint(keys[3], (BLOCK_SPAN_EAST, BLOCK_SPAN_NORTH, BLOCK_SPAN_UPWARD), BIN_CAPACITY // 8, BIN_CAPACITY + 1), jax.random.fold_in(keys[3], 1), BIN_CAPACITY // 8, BIN_CAPACITY).astype(jnp.int32),
    }


step_factor = 2.0

def conduct(fields, periodic_enclosure):
    extent_x, extent_y, extent_z = periodic_enclosure
    bin_dimensions = fields.shape[-1]

    def one_column(column):
        col_x = column // extent_y
        col_y = column % extent_y

        def column_at(shift_x, shift_y):
            column_part = lax.dynamic_slice_in_dim(fields, col_x + 1 + shift_x, 1, 1)
            column_part = lax.dynamic_slice_in_dim(column_part, col_y + 1 + shift_y, 1, 2)
            return column_part[:, 0, 0]
        target = column_at(0, 0)[:, 1:1 + extent_z]
        inflow = jnp.zeros((extent_z, bin_dimensions), jnp.float32)
        weights = jnp.zeros((extent_z, bin_dimensions), jnp.float32)
        for shift_x in (-1, 0, 1):
            for shift_y in (-1, 0, 1):
                source_col = column_at(shift_x, shift_y)
                for shift_z in (-1, 0, 1):
                    source = source_col[:, 1 + shift_z:1 + shift_z + extent_z]
                    dist_sq = (float(shift_x) + source[0][:, None, :] - target[0][:, :, None]) ** 2
                    dist_sq = dist_sq + (float(shift_y) + source[1][:, None, :] - target[1][:, :, None]) ** 2
                    dist_sq = dist_sq + (float(shift_z) + source[2][:, None, :] - target[2][:, :, None]) ** 2
                    kernel = jnp.maximum(1.0 - jnp.sqrt(dist_sq), 0.0) ** 3
                    pair = kernel * source[3][:, None, :] * (target[5][:, :, None] + source[5][:, None, :])
                    inflow = inflow + lax.optimization_barrier(jnp.sum(pair * (source[4][:, None, :] - target[4][:, :, None]), axis=2))
                    weights = weights + lax.optimization_barrier(jnp.sum(pair, axis=2))
        return (inflow, weights)
    inflow, weights = lax.map(one_column, jnp.arange(extent_x * extent_y, dtype=jnp.int32))
    array_shape = (extent_x, extent_y, extent_z, bin_dimensions)
    return (inflow.reshape(array_shape), weights.reshape(array_shape))

def wrap_fields(relative_placements, smoothed_particle_measure, temp, heat_diffusion_coefficient):
    fields = jnp.concatenate([relative_placements, smoothed_particle_measure[None], temp[None], heat_diffusion_coefficient[None]], axis=0)
    return jnp.pad(fields, ((0, 0), (1, 1), (1, 1), (1, 1), (0, 0)), mode='wrap')

def reference(relative_placements, mass_per_density, opening_heat_level, bin_fill_counts):
    bin_dimensions = opening_heat_level.shape[-1]
    occupied = (jnp.arange(bin_dimensions, dtype=jnp.int32)[None, None, None, :] < bin_fill_counts[..., None]).astype(jnp.float32)
    smoothed_particle_measure = mass_per_density * occupied
    heat_diffusion_coefficient = opening_heat_level ** 2.5
    periodic_enclosure = opening_heat_level.shape[:3]
    opening_index = opening_heat_level
    reference_heat_rate, row_sums = conduct(wrap_fields(relative_placements, smoothed_particle_measure, opening_index, heat_diffusion_coefficient), periodic_enclosure)
    super_interval_length = step_factor / jnp.max(row_sums * occupied)
    leading_subset = opening_index + 2.0 / 15.0 * super_interval_length * reference_heat_rate
    initial_flow, unused_one = conduct(wrap_fields(relative_placements, smoothed_particle_measure, leading_subset, heat_diffusion_coefficient), periodic_enclosure)
    second = 1.5 * leading_subset - 0.5 * opening_index + 0.6 * super_interval_length * initial_flow - 0.4 * super_interval_length * reference_heat_rate
    flow_second, unused_two = conduct(wrap_fields(relative_placements, smoothed_particle_measure, second, heat_diffusion_coefficient), periodic_enclosure)
    final_temp = 25.0 / 12.0 * second - 5.0 / 6.0 * leading_subset - 0.25 * opening_index + 5.0 / 6.0 * super_interval_length * flow_second - 5.0 / 9.0 * super_interval_length * reference_heat_rate
    return final_temp
```

```python
import functools
import itertools
import jax
import jax.numpy as jnp
from jax import lax
from jax.experimental import pallas as pl
from jax.experimental.pallas import tpu as pltpu
from jax.sharding import PartitionSpec as P

AXES = ("gx", "gy", "gz")
MESH = pl.DeviceIdType.MESH
f32, bf16 = jnp.float32, jnp.bfloat16
DIRS = [d for d in itertools.product((-1, 0, 1), repeat=3) if d != (0, 0, 0)]
COLUMNS = [(ex, ey) for ex in (-1, 0, 1) for ey in (-1, 0, 1)]


def split3(tile):
    hi = tile.astype(bf16).astype(f32)
    rest = tile - hi
    mid = rest.astype(bf16).astype(f32)
    return hi, mid, rest - mid


def kernel(dims, block, f_in, out, f_all, u1, u2, mx, mx_parts, fsend, frecv, usend, urecv, msend, mrecv):
    bx, by, bz = block
    lanes = f_in.shape[-1]
    me = [lax.axis_index(a) for a in AXES]
    row = lax.broadcasted_iota(jnp.int32, (8, lanes), 0)

    def neighbour(d):
        return tuple(lax.rem(me[k] + (d[k] + dims[k]), dims[k]) if d[k] else me[k] for k in range(3))

    def peer(axis, hop):
        return tuple(lax.rem(me[k] + hop, dims[k]) if k == axis else me[k] for k in range(3))

    barrier = pltpu.get_barrier_semaphore()
    count = 0
    for d in DIRS:
        pl.semaphore_signal(barrier, inc=1, device_id=neighbour(d), device_id_type=MESH)
        count += 1
    for axis in range(3):
        for hop in range(1, dims[axis]):
            pl.semaphore_signal(barrier, inc=1, device_id=peer(axis, hop), device_id_type=MESH)
            count += 1
    pl.semaphore_wait(barrier, count)

    def piece(d, base):
        src, dst = [], []
        for k in range(3):
            n = block[k]
            if d[k] == 0:
                src.append(pl.ds(base, n))
                dst.append(pl.ds(1, n))
            elif d[k] == 1:
                src.append(pl.ds(base + n - 1, 1))
                dst.append(pl.ds(0, 1))
            else:
                src.append(pl.ds(base, 1))
                dst.append(pl.ds(n + 1, 1))
        return tuple(src), tuple(dst)

    def halo_copies(src_ref, base, dst_ref, ssem, rsem):
        copies = []
        for i, d in enumerate(DIRS):
            src, dst = piece(d, base)
            copies.append(
                pltpu.make_async_remote_copy(
                    src_ref=src_ref.at[src],
                    dst_ref=dst_ref.at[dst],
                    send_sem=ssem.at[i],
                    recv_sem=rsem.at[i],
                    device_id=neighbour(d),
                    device_id_type=MESH,
                )
            )
        return copies

    def max_copies(axis):
        start = sum(dims[:axis])
        return [
            pltpu.make_async_remote_copy(
                src_ref=mx.at[axis],
                dst_ref=mx_parts.at[start + hop],
                send_sem=msend.at[start + hop],
                recv_sem=mrecv.at[start + hop],
                device_id=peer(axis, hop),
                device_id_type=MESH,
            )
            for hop in range(1, dims[axis])
        ]

    def start(copies):
        for c in copies:
            c.start()

    def wait(copies):
        for c in copies:
            c.wait()

    def max_result(axis):
        begin = sum(dims[:axis])
        total = mx[axis]
        for hop in range(1, dims[axis]):
            total = jnp.maximum(total, mx_parts[begin + hop])
        return total

    outer = tuple(n + 2 for n in block)
    pl.run_scoped(
        functools.partial(work, dims, block, f_in, out, f_all, u1, u2, mx, mx_parts, halo_copies, max_copies, max_result, start, wait, fsend, frecv, usend, urecv),
        pltpu.VMEM((bx * by * bz, 27, lanes, lanes), bf16),
        pltpu.VMEM(outer + (lanes, 48), bf16),
        pltpu.VMEM(block + (48, lanes), bf16),
        pltpu.VMEM(outer + (16, lanes), bf16),
    )


def work(dims, block, f_in, out, f_all, u1, u2, mx, mx_parts, halo_copies, max_copies, max_result, start, wait, fsend, frecv, usend, urecv, k_all, bt, at, w_all):
    bx, by, bz = block
    lanes = f_in.shape[-1]
    row = lax.broadcasted_iota(jnp.int32, (8, lanes), 0)
    first_halo = halo_copies(f_in, 0, f_all, fsend, frecv)
    start(first_halo)

    def place(col, carry):
        x, y = col // by, col % by
        for z in range(bz):
            f_all[x + 1, y + 1, z + 1] = f_in[x, y, z]
        return carry

    lax.fori_loop(0, bx * by, place, 0)

    def centred(x, y, z):
        cx = jnp.asarray(x, jnp.int32).astype(f32) - (0.5 * (bx + 1) + 0.5)
        cy = jnp.asarray(y, jnp.int32).astype(f32) - (0.5 * (by + 1) + 0.5)
        cz = z - (0.5 * (bz + 1) + 0.5)
        shift = jnp.where(row == 0, cx, jnp.where(row == 1, cy, cz))
        pos = jnp.where(row < 3, f_all[x, y, z] + shift, 0.0)
        return pos, jnp.sum(pos * pos, axis=0, keepdims=True)

    def source(x, y, z):
        pos, norm = centred(x, y, z)
        tile = jnp.where(row < 3, pos, jnp.where(row == 3, norm, jnp.where(row == 4, 1.0, 0.0)))
        hi, mid, lo = split3(tile)
        six = jnp.concatenate([hi, mid, hi, mid, lo, hi], axis=0)
        bt[x, y, z] = six.T.astype(bf16)

    def own_sources(col, carry):
        for z in range(bz):
            source(col // by + 1, col % by + 1, z + 1)
        return carry

    lax.fori_loop(0, bx * by, own_sources, 0)

    def targets(col, carry):
        x, y = col // by, col % by
        for z in range(bz):
            pos, norm = centred(x + 1, y + 1, z + 1)
            tile = jnp.where(row < 3, -2.0 * pos, jnp.where(row == 3, 1.0, jnp.where(row == 4, norm, 0.0)))
            hi, mid, lo = split3(tile)
            at[x, y, z] = jnp.concatenate([hi, hi, mid, mid, hi, lo], axis=0).astype(bf16)
        return carry

    lax.fori_loop(0, bx * by, targets, 0)

    def spread(dist_sq):
        dist_sq = jnp.maximum(dist_sq, 1e-12)
        near = (1.0 - dist_sq * lax.rsqrt(dist_sq)).astype(bf16)
        near = jnp.maximum(near, jnp.zeros((), bf16))
        return near * near * near

    same = lax.broadcasted_iota(jnp.int32, (lanes, lanes), 0) == lax.broadcasted_iota(
        jnp.int32, (lanes, lanes), 1
    )

    def pairs(x, y, sx, sy, c, own, ends):
        for zp in range(bz // 2):
            z = 2 * zp
            both = jnp.concatenate([at[x, y, z], at[x, y, z + 1]], axis=1)
            for s in range(4):
                rim = (zp == 0 and s == 0) or (zp == bz // 2 - 1 and s == 3)
                if rim != ends:
                    continue
                lo_t, hi_t = max(s - 2, 0), min(s, 1)
                a = both[:, lo_t * lanes : (hi_t + 1) * lanes]
                d2 = jnp.dot(bt[sx, sy, z + s], a, preferred_element_type=f32)
                for which in range(lo_t, hi_t + 1):
                    part = d2[:, (which - lo_t) * lanes : (which - lo_t + 1) * lanes]
                    if own and s == which + 1:
                        part = jnp.where(same, 0.0, part)
                    k_all[(x * by + y) * bz + z + which, c * 3 + s - which] = spread(part)

    for c, (ex, ey) in enumerate(COLUMNS):
        nx, ny = bx - abs(ex), by - abs(ey)
        group = 3 if nx * ny % 3 == 0 else 2 if nx * ny % 2 == 0 else 1

        def inner(step, carry, c=c, ex=ex, ey=ey, ny=ny, group=group):
            for k in range(group):
                i = step * group + k
                x, y = max(0, -ex) + i // ny, max(0, -ey) + i % ny
                pairs(x, y, x + 1 + ex, y + 1 + ey, c, (ex, ey) == (0, 0), False)
            return carry

        lax.fori_loop(0, nx * ny // group, inner, 0)

    wait(first_halo)

    def rim_sources(col, carry):
        for z in range(bz + 2):
            source(col // (by + 2), col % (by + 2), z)
        return carry

    lax.fori_loop(0, (bx + 2) * (by + 2), rim_sources, 0)

    for side in (-1, 1):

        def rim_x(e, carry, side=side):
            x = bx - 1 if side == 1 else 0
            for y in range(by):
                pairs(x, y, x + 1 + side, y + e, (side + 1) * 3 + e, False, False)
            return carry

        def rim_y(e, carry, side=side):
            y = by - 1 if side == 1 else 0
            for x in range(bx):
                pairs(x, y, x + e, y + 1 + side, e * 3 + side + 1, False, False)
            return carry

        lax.fori_loop(0, 3, rim_x, 0)
        lax.fori_loop(0, 3, rim_y, 0)

    def ends(col, carry):
        x, y = col // by, col % by
        for c, (ex, ey) in enumerate(COLUMNS):
            pairs(x, y, x + 1 + ex, y + 1 + ey, c, False, True)
        return carry

    lax.fori_loop(0, bx * by, ends, 0)

    def weigh(u_of):
        def body(col, carry):
            x, y = col // (by + 2), col % (by + 2)
            for z in range(bz + 2):
                tile = f_all[x, y, z]
                v, c = tile[3:4], tile[5:6]
                coef = jnp.where(row < 4, jnp.where(row % 2 == 0, v, v * c), 0.0)
                coef = coef * jnp.where(row < 2, u_of(x, y, z), 1.0)
                hi = coef.astype(bf16).astype(f32)
                w_all[x, y, z] = jnp.concatenate([hi, coef - hi], axis=0).astype(bf16)
            return carry

        lax.fori_loop(0, (bx + 2) * (by + 2), body, 0)

    def apply(u_of, emit, init):
        def body(col, carry):
            x, y = col // by, col % by
            for z in range(bz):
                w = jnp.concatenate(
                    [w_all[x + 1 + ex, y + 1 + ey, z + ez] for ex, ey in COLUMNS for ez in range(3)], axis=1
                )
                block_k = k_all[col * bz + z].reshape(27 * lanes, lanes)
                o = jnp.dot(w, block_k, preferred_element_type=f32)
                o = o[0:8] + o[8:16]
                u = u_of(x + 1, y + 1, z + 1)
                c = f_all[x + 1, y + 1, z + 1, 5:6]
                flow = c * (o[0:1] - u * o[2:3]) + (o[1:2] - u * o[3:4])
                carry = emit(carry, x, y, z, flow, c * o[2:3] + o[3:4])
            return carry

        return lax.fori_loop(0, bx * by, body, init)

    def u0_of(x, y, z):
        return f_all[x, y, z, 4:5]

    def u1_of(x, y, z):
        return u1[x, y, z]

    def u2_of(x, y, z):
        return u2[x, y, z]

    def emit0(carry, x, y, z, flow, rows):
        u1[x + 1, y + 1, z + 1] = flow
        return jnp.maximum(carry, rows * f_all[x + 1, y + 1, z + 1, 6:7])

    weigh(u0_of)
    largest = apply(u0_of, emit0, jnp.zeros((1, lanes), f32))
    mx[0] = jnp.broadcast_to(largest, (8, lanes))
    halo1 = halo_copies(u1, 1, u1, usend.at[0], urecv.at[0])
    max0 = max_copies(0)
    start(halo1)
    start(max0)
    wait(halo1)
    wait(max0)
    mx[1] = max_result(0)
    max1 = max_copies(1)
    start(max1)

    def emit1(carry, x, y, z, flow, rows):
        u2[x + 1, y + 1, z + 1] = flow
        return carry

    weigh(u1_of)
    apply(u1_of, emit1, 0)
    halo2 = halo_copies(u2, 1, u2, usend.at[1], urecv.at[1])
    start(halo2)
    wait(max1)
    mx[2] = max_result(1)
    max2 = max_copies(2)
    start(max2)
    wait(halo2)
    wait(max2)
    step = 2.0 / jnp.max(max_result(2)[0:1], axis=1, keepdims=True)

    def emit2(carry, x, y, z, f2, rows):
        u0 = f_all[x + 1, y + 1, z + 1, 4:5]
        f0, f1 = u1[x + 1, y + 1, z + 1], u2[x + 1, y + 1, z + 1]
        first = u0 + 2.0 / 15.0 * step * f0
        l_first = f0 + 2.0 / 15.0 * step * f1
        l_l_first = f1 + 2.0 / 15.0 * step * f2
        second = 1.5 * first - 0.5 * u0 + 0.6 * step * l_first - 0.4 * step * f0
        l_second = 1.5 * l_first - 0.5 * f0 + 0.6 * step * l_l_first - 0.4 * step * f1
        out[x, y, z] = (
            25.0 / 12.0 * second
            - 5.0 / 6.0 * first
            - 0.25 * u0
            + 5.0 / 6.0 * step * l_second
            - 5.0 / 9.0 * step * f0
        )
        return carry

    weigh(u2_of)
    apply(u2_of, emit2, 0)


def local(relative_placements, mass_per_density, opening_heat_level, bin_fill_counts):
    lanes = opening_heat_level.shape[-1]
    block = opening_heat_level.shape[:3]
    dims = tuple(lax.axis_size(a) for a in AXES)
    occupied = (
        jnp.arange(lanes, dtype=jnp.int32)[None, None, None, :] < bin_fill_counts[..., None]
    ).astype(f32)
    heat = opening_heat_level
    rows = [relative_placements[0], relative_placements[1], relative_placements[2]]
    rows += [mass_per_density * occupied, heat, heat * heat * jnp.sqrt(heat), occupied, jnp.zeros_like(heat)]
    fields = jnp.stack(rows, axis=3)
    outer = tuple(n + 2 for n in block)
    cells = block[0] * block[1] * block[2]
    vmem = pl.BlockSpec(memory_space=pltpu.VMEM)
    dma = pltpu.SemaphoreType.DMA
    n_dirs = len(DIRS)
    final = pl.pallas_call(
        functools.partial(kernel, dims, block),
        out_shape=jax.ShapeDtypeStruct(block + (1, lanes), f32),
        in_specs=[vmem],
        out_specs=vmem,
        scratch_shapes=[
            pltpu.VMEM(outer + (8, lanes), f32),
            pltpu.VMEM(outer + (1, lanes), f32),
            pltpu.VMEM(outer + (1, lanes), f32),
            pltpu.VMEM((3, 8, lanes), f32),
            pltpu.VMEM((sum(dims), 8, lanes), f32),
            dma((n_dirs,)),
            dma((n_dirs,)),
            dma((2, n_dirs)),
            dma((2, n_dirs)),
            dma((sum(dims),)),
            dma((sum(dims),)),
        ],
        compiler_params=pltpu.CompilerParams(
            collective_id=0, has_side_effects=True, vmem_limit_bytes=60 * 1024 * 1024
        ),
    )(fields)
    return final.reshape(heat.shape)


def solution(mesh):
    in_specs = (
        P(None, "gx", "gy", "gz", None),
        P("gx", "gy", "gz", None),
        P("gx", "gy", "gz", None),
        P("gx", "gy", "gz"),
    )
    out_specs = P("gx", "gy", "gz", None)
    return jax.shard_map(local, mesh=mesh, in_specs=in_specs, out_specs=out_specs, check_vma=False)
```

```python
import functools
import itertools
import jax
import jax.numpy as jnp
from jax import lax
from jax.experimental import pallas as pl
from jax.experimental.pallas import tpu as pltpu
from jax.sharding import PartitionSpec as P

AXES = ("gx", "gy", "gz")
MESH = pl.DeviceIdType.MESH
f32, bf16 = jnp.float32, jnp.bfloat16
DIRS = [d for d in itertools.product((-1, 0, 1), repeat=3) if d != (0, 0, 0)]
ROWS = 8
HEAT = 4


def split3(tile):
    hi = tile.astype(bf16).astype(f32)
    rest = tile - hi
    mid = rest.astype(bf16).astype(f32)
    return hi, mid, rest - mid


def split2(tile):
    hi = tile.astype(bf16).astype(f32)
    return hi, tile - hi


def kernel(dims, block, counts, offsets, mass, heat, out, f_own, f_all, u_own, u_all, mx, mx_parts, fsend, frecv, usend, urecv, msend, mrecv):
    bx, by, bz = block
    lanes = heat.shape[-1]
    me = [lax.axis_index(a) for a in AXES]

    def neighbour(d):
        return tuple(lax.rem(me[k] + (d[k] + dims[k]), dims[k]) if d[k] else me[k] for k in range(3))

    def peer(axis, hop):
        return tuple(lax.rem(me[k] + hop, dims[k]) if k == axis else me[k] for k in range(3))

    barrier = pltpu.get_barrier_semaphore()
    count = 0
    for d in DIRS:
        pl.semaphore_signal(barrier, inc=1, device_id=neighbour(d), device_id_type=MESH)
        count += 1
    for axis in range(3):
        for hop in range(1, dims[axis]):
            pl.semaphore_signal(barrier, inc=1, device_id=peer(axis, hop), device_id_type=MESH)
            count += 1

    row = lax.broadcasted_iota(jnp.int32, (ROWS, lanes), 0)
    lane = lax.broadcasted_iota(jnp.int32, (ROWS, lanes), 1)
    zero = jnp.zeros((ROWS, lanes), f32)

    def own_rows(tile):
        pad = [jnp.zeros((1, lanes), f32), tile, jnp.zeros((ROWS - 1 - bz, lanes), f32)]
        return jnp.concatenate(pad, axis=0)

    def load_own(x, carry):
        for y in range(by):
            filled = jnp.zeros((ROWS, lanes), jnp.int32)
            for z in range(bz):
                filled = jnp.where(row == z + 1, counts[x, y, z], filled)
            parts = [offsets[0, x, y], offsets[1, x, y], offsets[2, x, y], mass[x, y], heat[x, y]]
            for k, part in enumerate(parts):
                tile = own_rows(part)
                if k == 3:
                    tile = jnp.where(lane < filled, tile, 0.0)
                f_own[k, x, y] = tile
                f_all[k, x + 1, y + 1, 1 : bz + 1] = tile[1 : bz + 1]
        return carry

    lax.fori_loop(0, bx, load_own, 0)
    pl.semaphore_wait(barrier, count)

    def piece(d):
        src, dst = [], []
        for k in range(3):
            n, base = block[k], 1 if k == 2 else 0
            if d[k] == 0:
                src.append(pl.ds(base, n))
                dst.append(pl.ds(1, n))
            elif d[k] == 1:
                src.append(pl.ds(base + n - 1, 1))
                dst.append(pl.ds(0, 1))
            else:
                src.append(pl.ds(base, 1))
                dst.append(pl.ds(n + 1, 1))
        return tuple(src), tuple(dst)

    def halo_copies(src_ref, lead_src, dst_ref, lead_dst, ssem, rsem):
        copies = []
        for i, d in enumerate(DIRS):
            src, dst = piece(d)
            copies.append(
                pltpu.make_async_remote_copy(
                    src_ref=src_ref.at[(lead_src,) + src],
                    dst_ref=dst_ref.at[(lead_dst,) + dst],
                    send_sem=ssem.at[i],
                    recv_sem=rsem.at[i],
                    device_id=neighbour(d),
                    device_id_type=MESH,
                )
            )
        return copies

    def max_copies(axis):
        start = sum(dims[:axis])
        return [
            pltpu.make_async_remote_copy(
                src_ref=mx.at[axis],
                dst_ref=mx_parts.at[start + hop],
                send_sem=msend.at[start + hop],
                recv_sem=mrecv.at[start + hop],
                device_id=peer(axis, hop),
                device_id_type=MESH,
            )
            for hop in range(1, dims[axis])
        ]

    def max_result(axis):
        begin = sum(dims[:axis])
        total = mx[axis]
        for hop in range(1, dims[axis]):
            total = jnp.maximum(total, mx_parts[begin + hop])
        return total

    fields = pl.ds(0, f_own.shape[0])
    first_halo = halo_copies(f_own, fields, f_all, fields, fsend, frecv)
    for c in first_halo:
        c.start()

    def halo(step):
        return halo_copies(u_own, step, u_all, step, usend.at[step], urecv.at[step])

    sides = (bx + 2) * (by + 2)
    body = functools.partial(
        work, block, lanes, f_own, f_all, u_own, u_all, mx, out, counts, first_halo, halo, max_copies, max_result
    )
    tiles = 22 * ROWS
    group = (3 * by - 2) * 2
    pl.run_scoped(
        body,
        pltpu.VMEM((bx * by * bz, 27, lanes, lanes), bf16),
        pltpu.VMEM((sides, lanes, tiles), bf16),
        pltpu.VMEM((bx * by, bz // 2, 3, tiles, 2 * lanes), bf16),
        pltpu.VMEM((max(group, 6 * by), lanes, 2 * lanes), f32),
        pltpu.VMEM((max(group, 6 * by), lanes, 2 * lanes), f32),
        pltpu.VMEM((sides, 3, 8 * ROWS, lanes), bf16),
        pltpu.VMEM((sides, 3, 4 * ROWS, lanes), bf16),
        pltpu.VMEM((sides, 2, ROWS, lanes), f32),
        pltpu.VMEM((bx * by, 4, ROWS, lanes), f32),
        pltpu.VMEM((bx * by, 2, ROWS, lanes), f32),
    )


def work(block, lanes, f_own, f_all, u_own, u_all, mx, out, counts, first_halo, halo, max_copies, max_result,
         k_all, bt, at, buf_a, buf_b, w0_all, w_all, vol, acc, sums):
    bx, by, bz = block
    nx, ny = bx + 2, by + 2
    row = lax.broadcasted_iota(jnp.int32, (ROWS, lanes), 0)
    inside = (row >= 1) & (row <= bz)
    known = row <= bz + 1
    last = ROWS - 1

    def start(copies):
        for c in copies:
            c.start()

    def wait(copies):
        for c in copies:
            c.wait()

    def centred(px, py, pz, x, y):
        cx = jnp.asarray(x, jnp.int32).astype(f32) - (0.5 * (bx + 1) + 0.5)
        cy = jnp.asarray(y, jnp.int32).astype(f32) - (0.5 * (by + 1) + 0.5)
        cz = row.astype(f32) - (0.5 * (bz + 1) + 0.5)
        px, py, pz = px + cx, py + cy, pz + cz
        return (px, py, pz), px * px + py * py + pz * pz

    def source(col, x, y, tile_of):
        pos, norm = centred(tile_of(0), tile_of(1), tile_of(2), x, y)
        parts = []
        for p in pos:
            hi, mid, lo = split3(p)
            parts += [hi, mid, hi, mid, lo, hi]
        parts += [jnp.where(row == last, 1.0, part) for part in split3(norm)]
        parts.append(jnp.zeros((ROWS, lanes), f32))
        stack = jnp.concatenate(parts, axis=0).astype(bf16)
        bt[col] = stack.T

    def own_sources(x, carry):
        for y in range(by):
            source((x + 1) * ny + y + 1, x + 1, y + 1, lambda k, y=y: f_own[k, x, y])
        return carry

    lax.fori_loop(0, bx, own_sources, 0)

    def targets(x, carry):
        for y in range(by):
            pos, norm = centred(f_own[0, x, y], f_own[1, x, y], f_own[2, x, y], x + 1, y + 1)
            coefs = [split3(-2.0 * p) for p in pos]
            norms = split3(norm)
            moved = [[[pltpu.roll(part, ez % ROWS, 0) if ez else part for part in c] for c in coefs] for ez in (-1, 0, 1)]
            for zp in range(bz // 2):
                for ez in (-1, 0, 1):
                    halves = []
                    for t in (2 * zp + 1, 2 * zp + 2):
                        here = row == t + ez
                        parts = []
                        for c in moved[ez + 1]:
                            hi, mid, lo = [jnp.where(here, part, 0.0) for part in c]
                            parts += [hi, hi, mid, mid, hi, lo]
                        for part in norms:
                            at_last = pltpu.roll(part, last - t, 0)
                            parts.append(jnp.where(here, 1.0, jnp.where(row == last, at_last, 0.0)))
                        parts.append(jnp.zeros((ROWS, lanes), f32))
                        halves.append(jnp.concatenate(parts, axis=0).astype(bf16))
                    at[x * by + y, zp, ez + 1] = jnp.concatenate(halves, axis=1)
        return carry

    lax.fori_loop(0, bx, targets, 0)

    def unit(x, y, cx, cy, zp, ez):
        return dict(t=x * by + y, c=(cx + 1) * ny + cy + 1, zp=zp, ez=ez, slot=((cx - x + 1) * 3 + cy - y + 1) * 3 + ez + 1)

    def gemm(buf, units):
        for i, u in enumerate(units):
            buf[i] = jnp.dot(bt[u["c"]], at[u["t"], u["zp"], u["ez"] + 1], preferred_element_type=f32)

    def spread(buf, units):
        for i, u in enumerate(units):
            for half in range(2):
                dist_sq = jnp.maximum(buf[i, :, half * lanes : (half + 1) * lanes], 1e-12)
                near = (1.0 - dist_sq * lax.rsqrt(dist_sq)).astype(bf16)
                near = jnp.maximum(near, jnp.zeros((), bf16))
                k_all[u["t"] * bz + 2 * u["zp"] + half, u["slot"]] = near * near * near

    def pipeline(trips, first, second, extra=None):
        gemm(buf_a, first(0))

        def step(i, carry):
            gemm(buf_b, second(i))
            spread(buf_a, first(i))
            gemm(buf_a, first(jnp.minimum(i + 1, trips - 1)))
            spread(buf_b, second(i))
            if extra is not None:
                extra(i)
            return carry

        lax.fori_loop(0, trips, step, 0)

    y_pairs = [(y, cy) for y in range(by) for cy in (y - 1, y, y + 1) if 0 <= cy < by]
    y_rims = [(0, -1), (by - 1, by)]
    n_pairs = 3 * bx - 2
    halves = range(bz // 2)

    def x_pair(k):
        x = (k + 1) // 3
        return x, k - 2 * x

    def own_units(zp):
        ezs = [ez for ez in (-1, 0, 1) if 0 <= 2 * zp + ez and 2 * zp + 1 + ez < bz]

        def units(k):
            x, cx = x_pair(k)
            return [unit(x, y, cx, cy, zp, ez) for y, cy in y_pairs for ez in ezs]

        return units

    def rim_units(zp):
        ezs = [ez for ez in (-1, 0, 1) if not (0 <= 2 * zp + ez and 2 * zp + 1 + ez < bz)]

        def units(k):
            x, cx = x_pair(k)
            return [unit(x, y, cx, cy, zp, ez) for y, cy in y_pairs for ez in ezs] + [
                unit(x, y, cx, cy, zp, ez) for y, cy in y_rims for ez in (-1, 0, 1)
            ]

        return units

    def far_units(zp):
        def units(y):
            return [
                unit(x, y, cx, y + ey, zp, ez)
                for x, cx in ((0, -1), (bx - 1, bx))
                for ey in (-1, 0, 1)
                for ez in (-1, 0, 1)
            ]

        return units

    pipeline(n_pairs, own_units(0), own_units(1))

    same = lax.broadcasted_iota(jnp.int32, (lanes, lanes), 0) == lax.broadcasted_iota(jnp.int32, (lanes, lanes), 1)
    same = same.astype(f32).astype(bf16)

    def itself(t, carry):
        for z in range(bz):
            k_all[t * bz + z, 13] = jnp.maximum(k_all[t * bz + z, 13], same)
        return carry

    lax.fori_loop(0, bx * by, itself, 0)

    wait(first_halo)

    def all_sources(x, carry):
        for y in range(ny):
            source(x * ny + y, x, y, lambda k, y=y: jnp.where(known, f_all[k, x, y], 0.0))
        return carry

    lax.fori_loop(0, nx, all_sources, 0)

    def shifted(ref, col, kinds):
        his, los = zip(*[split2(k) for k in kinds])
        for ez in (-1, 0, 1):
            parts = [pltpu.roll(p, -ez % ROWS, 0) if ez else p for p in his + los]
            ref[col, ez + 1] = jnp.concatenate(parts, axis=0).astype(bf16)

    def weigh_first(x, carry):
        for y in range(ny):
            col = x * ny + y
            v, u = f_all[3, x, y], f_all[HEAT, x, y]
            vc = v * (u * u * jnp.sqrt(u))
            vol[col, 0] = v
            vol[col, 1] = vc
            shifted(w0_all, col, [v, vc, v * u, vc * u])
        return carry

    lax.fori_loop(0, nx, weigh_first, 0)
    pipeline(n_pairs, rim_units(0), rim_units(1))
    pipeline(by, far_units(0), far_units(1))

    def reduce(w_ref, kinds, x, y, lists):
        total = jnp.zeros((kinds * ROWS, lanes), f32)
        wide = lax.broadcasted_iota(jnp.int32, (kinds * ROWS, lanes), 0) % ROWS
        for z in range(bz):
            items = [(cx, cy, ez) for cx, cy, ez in lists[z]]
            if not items:
                continue
            w = jnp.concatenate([w_ref[(cx + 1) * ny + cy + 1, ez + 1] for cx, cy, ez in items], axis=1)
            k = jnp.concatenate(
                [k_all[(x * by + y) * bz + z, ((cx - x + 1) * 3 + cy - y + 1) * 3 + ez + 1] for cx, cy, ez in items], axis=0
            )
            o = jnp.dot(w, k, preferred_element_type=f32)
            o = o[: kinds * ROWS] + o[kinds * ROWS :]
            total = jnp.where(wide == z + 1, o, total)
        return total

    def flow_of(s_vu, s_vcu, s_v, s_vc, u, c):
        return c * (s_vu - u * s_v) + (s_vcu - u * s_vc)

    def heat_power(u):
        return u * u * jnp.sqrt(u)

    def emit(step, x, y, flow):
        u_own[step, x, y] = flow
        u_all[step, x + 1, y + 1, 1 : bz + 1] = flow[1 : bz + 1]

    every = [[(ex, ey, ez) for ex in (-1, 0, 1) for ey in (-1, 0, 1) for ez in (-1, 0, 1)] for z in range(bz)]

    def apply_first(x, largest):
        for y in range(by):
            lists = [[(x + ex, y + ey, ez) for ex, ey, ez in every[z]] for z in range(bz)]
            o = reduce(w0_all, 4, x, y, lists)
            s_v, s_vc, s_vu, s_vcu = [o[k * ROWS : (k + 1) * ROWS] for k in range(4)]
            u = f_own[HEAT, x, y]
            c = heat_power(u)
            sums[x * by + y, 0] = s_v
            sums[x * by + y, 1] = s_vc
            emit(0, x, y, jnp.where(inside, flow_of(s_vu, s_vcu, s_v, s_vc, u, c), 0.0))
            rows = c * s_v + s_vc
            lane = lax.broadcasted_iota(jnp.int32, (ROWS, lanes), 1)
            filled = jnp.zeros((ROWS, lanes), jnp.int32)
            for z in range(bz):
                filled = jnp.where(row == z + 1, counts[x, y, z], filled)
            largest = jnp.maximum(largest, jnp.where(lane < filled, rows, 0.0))
        return largest

    mx[0] = lax.fori_loop(0, bx, apply_first, jnp.zeros((ROWS, lanes), f32))
    halo1 = halo(0)
    max0 = max_copies(0)
    start(halo1)
    start(max0)

    def weigh_own(step):
        def body(x, carry):
            for y in range(by):
                col = (x + 1) * ny + y + 1
                u = u_own[step, x, y]
                shifted(w_all, col, [vol[col, 0] * u, vol[col, 1] * u])
            return carry

        lax.fori_loop(0, bx, body, 0)

    def weigh_all(step):
        def body(x, carry):
            for y in range(ny):
                col = x * ny + y
                u = u_all[step, x, y]
                shifted(w_all, col, [vol[col, 0] * u, vol[col, 1] * u])
            return carry

        lax.fori_loop(0, nx, body, 0)

    def add(x, y, o, first=False):
        for k in range(2):
            part = o[k * ROWS : (k + 1) * ROWS]
            acc[x * by + y, k] = part if first else acc[x * by + y, k] + part

    def apply_own(step):
        for x in range(bx):
            for y in range(by):
                for k in range(2):
                    acc[x * by + y, k] = jnp.zeros((ROWS, lanes), f32)
        weigh_own(step)

        def body(k, carry):
            x, cx = x_pair(k)
            for y in range(by):
                lists = [
                    [(cx, cy, ez) for yy, cy in y_pairs if yy == y for ez in (-1, 0, 1) if 0 <= z + ez < bz] for z in range(bz)
                ]
                add(x, y, reduce(w_all, 2, x, y, lists))
            return carry

        lax.fori_loop(0, n_pairs, body, 0)

    def apply_rest(step):
        weigh_all(step)

        def rim(k, carry):
            x, cx = x_pair(k)
            for y in range(by):
                lists = [
                    [(cx, cy, ez) for yy, cy in y_pairs if yy == y for ez in (-1, 0, 1) if not 0 <= z + ez < bz]
                    + [(cx, cy, ez) for yy, cy in y_rims if yy == y for ez in (-1, 0, 1)]
                    for z in range(bz)
                ]
                add(x, y, reduce(w_all, 2, x, y, lists))
            return carry

        lax.fori_loop(0, n_pairs, rim, 0)

        def far(y, carry):
            for x, cx in ((0, -1), (bx - 1, bx)):
                lists = [[(cx, y + ey, ez) for ey in (-1, 0, 1) for ez in (-1, 0, 1)] for z in range(bz)]
                add(x, y, reduce(w_all, 2, x, y, lists))
            return carry

        lax.fori_loop(0, by, far, 0)

    def flow_at(step, x, y):
        t = x * by + y
        u = u_own[step, x, y]
        return flow_of(acc[t, 0], acc[t, 1], sums[t, 0], sums[t, 1], u, heat_power(f_own[HEAT, x, y]))

    apply_own(0)
    wait(halo1)
    wait(max0)
    mx[1] = max_result(0)
    max1 = max_copies(1)
    start(max1)
    apply_rest(0)
    for x in range(bx):
        for y in range(by):
            emit(1, x, y, jnp.where(inside, flow_at(0, x, y), 0.0))
    halo2 = halo(1)
    start(halo2)
    wait(max1)
    mx[2] = max_result(1)
    max2 = max_copies(2)
    start(max2)
    apply_own(1)
    wait(halo2)
    wait(max2)
    apply_rest(1)
    top = jnp.max(jnp.max(max_result(2), axis=1, keepdims=True), axis=0, keepdims=True)
    step = 2.0 / top
    for x in range(bx):
        for y in range(by):
            f2 = flow_at(1, x, y)
            u0, f0, f1 = f_own[HEAT, x, y], u_own[0, x, y], u_own[1, x, y]
            first = u0 + 2.0 / 15.0 * step * f0
            l_first = f0 + 2.0 / 15.0 * step * f1
            l_l_first = f1 + 2.0 / 15.0 * step * f2
            second = 1.5 * first - 0.5 * u0 + 0.6 * step * l_first - 0.4 * step * f0
            l_second = 1.5 * l_first - 0.5 * f0 + 0.6 * step * l_l_first - 0.4 * step * f1
            final = (
                25.0 / 12.0 * second
                - 5.0 / 6.0 * first
                - 0.25 * u0
                + 5.0 / 6.0 * step * l_second
                - 5.0 / 9.0 * step * f0
            )
            out[x, y] = final[1 : bz + 1]


def local(relative_placements, mass_per_density, opening_heat_level, bin_fill_counts):
    lanes = opening_heat_level.shape[-1]
    block = opening_heat_level.shape[:3]
    dims = tuple(lax.axis_size(a) for a in AXES)
    bx, by, bz = block
    vmem = pl.BlockSpec(memory_space=pltpu.VMEM)
    dma = pltpu.SemaphoreType.DMA
    n_dirs = len(DIRS)
    return pl.pallas_call(
        functools.partial(kernel, dims, block),
        out_shape=jax.ShapeDtypeStruct(block + (lanes,), f32),
        in_specs=[pl.BlockSpec(memory_space=pltpu.SMEM), vmem, vmem, vmem],
        out_specs=vmem,
        scratch_shapes=[
            pltpu.VMEM((HEAT + 1, bx, by, ROWS, lanes), f32),
            pltpu.VMEM((HEAT + 1, bx + 2, by + 2, ROWS, lanes), f32),
            pltpu.VMEM((2, bx, by, ROWS, lanes), f32),
            pltpu.VMEM((2, bx + 2, by + 2, ROWS, lanes), f32),
            pltpu.VMEM((3, ROWS, lanes), f32),
            pltpu.VMEM((sum(dims), ROWS, lanes), f32),
            dma((n_dirs,)),
            dma((n_dirs,)),
            dma((2, n_dirs)),
            dma((2, n_dirs)),
            dma((sum(dims),)),
            dma((sum(dims),)),
        ],
        compiler_params=pltpu.CompilerParams(
            collective_id=0, has_side_effects=True, vmem_limit_bytes=60 * 1024 * 1024
        ),
    )(bin_fill_counts, relative_placements, mass_per_density, opening_heat_level)


def solution(mesh):
    in_specs = (
        P(None, "gx", "gy", "gz", None),
        P("gx", "gy", "gz", None),
        P("gx", "gy", "gz", None),
        P("gx", "gy", "gz"),
    )
    out_specs = P("gx", "gy", "gz", None)
    return jax.shard_map(local, mesh=mesh, in_specs=in_specs, out_specs=out_specs, check_vma=False)
```

```python
import functools
import itertools
import jax
import jax.numpy as jnp
from jax import lax
from jax.experimental import pallas as pl
from jax.experimental.pallas import tpu as pltpu
from jax.sharding import PartitionSpec as P

AXES = ("gx", "gy", "gz")
MESH = pl.DeviceIdType.MESH
f32, bf16 = jnp.float32, jnp.bfloat16
DIRS = [d for d in itertools.product((-1, 0, 1), repeat=3) if d != (0, 0, 0)]
ROWS = 8
HEAT = 4


def split3(tile):
    hi = tile.astype(bf16).astype(f32)
    rest = tile - hi
    mid = rest.astype(bf16).astype(f32)
    return hi, mid, rest - mid


def split2(tile):
    hi = tile.astype(bf16).astype(f32)
    return hi, tile - hi


def padded(tile):
    lanes = tile.shape[-1]
    pad = [jnp.zeros((1, lanes), f32), tile, jnp.zeros((ROWS - 1 - tile.shape[0], lanes), f32)]
    return jnp.concatenate(pad, axis=0)


def kernel(dims, block, counts, offsets, mass, heat, out, f_own, f_all, u_own, u_all, mx, mx_parts, fsend, frecv, usend, urecv, msend, mrecv):
    bx, by, bz = block
    lanes = heat.shape[-1]
    me = [lax.axis_index(a) for a in AXES]

    def neighbour(d):
        return tuple(lax.rem(me[k] + (d[k] + dims[k]), dims[k]) if d[k] else me[k] for k in range(3))

    def peer(axis, hop):
        return tuple(lax.rem(me[k] + hop, dims[k]) if k == axis else me[k] for k in range(3))

    barrier = pltpu.get_barrier_semaphore()
    count = 0
    for d in DIRS:
        pl.semaphore_signal(barrier, inc=1, device_id=neighbour(d), device_id_type=MESH)
        count += 1
    for axis in range(3):
        for hop in range(1, dims[axis]):
            pl.semaphore_signal(barrier, inc=1, device_id=peer(axis, hop), device_id_type=MESH)
            count += 1

    row = lax.broadcasted_iota(jnp.int32, (ROWS, lanes), 0)
    lane = lax.broadcasted_iota(jnp.int32, (ROWS, lanes), 1)
    zero = jnp.zeros((ROWS, lanes), f32)

    def load_own(x, carry):
        for y in range(by):
            filled = jnp.zeros((ROWS, lanes), jnp.int32)
            for z in range(bz):
                filled = jnp.where(row == z + 1, counts[x, y, z], filled)
            parts = [offsets[0, x, y], offsets[1, x, y], offsets[2, x, y], mass[x, y], heat[x, y]]
            for k, part in enumerate(parts):
                tile = padded(part)
                if k == 3:
                    tile = jnp.where(lane < filled, tile, 0.0)
                f_own[k, x, y] = tile
                f_all[k, x + 1, y + 1, 1 : bz + 1] = tile[1 : bz + 1]
        return carry

    lax.fori_loop(0, bx, load_own, 0)

    def piece(d):
        src, dst = [], []
        for k in range(3):
            n, base = block[k], 1 if k == 2 else 0
            if d[k] == 0:
                src.append(pl.ds(base, n))
                dst.append(pl.ds(1, n))
            elif d[k] == 1:
                src.append(pl.ds(base + n - 1, 1))
                dst.append(pl.ds(0, 1))
            else:
                src.append(pl.ds(base, 1))
                dst.append(pl.ds(n + 1, 1))
        return tuple(src), tuple(dst)

    def halo_copies(src_ref, lead_src, dst_ref, lead_dst, ssem, rsem):
        copies = []
        for i, d in enumerate(DIRS):
            src, dst = piece(d)
            copies.append(
                pltpu.make_async_remote_copy(
                    src_ref=src_ref.at[(lead_src,) + src],
                    dst_ref=dst_ref.at[(lead_dst,) + dst],
                    send_sem=ssem.at[i],
                    recv_sem=rsem.at[i],
                    device_id=neighbour(d),
                    device_id_type=MESH,
                )
            )
        return copies

    def max_copies(axis):
        start = sum(dims[:axis])
        return [
            pltpu.make_async_remote_copy(
                src_ref=mx.at[axis],
                dst_ref=mx_parts.at[start + hop],
                send_sem=msend.at[start + hop],
                recv_sem=mrecv.at[start + hop],
                device_id=peer(axis, hop),
                device_id_type=MESH,
            )
            for hop in range(1, dims[axis])
        ]

    def max_result(axis):
        begin = sum(dims[:axis])
        total = mx[axis]
        for hop in range(1, dims[axis]):
            total = jnp.maximum(total, mx_parts[begin + hop])
        return total

    fields = pl.ds(0, f_own.shape[0])
    first_halo = halo_copies(f_own, fields, f_all, fields, fsend, frecv)

    def greet():
        pl.semaphore_wait(barrier, count)
        for c in first_halo:
            c.start()

    def halo(step):
        return halo_copies(u_own, step, u_all, step, usend.at[step], urecv.at[step])

    sides = (bx + 2) * (by + 2)
    body = functools.partial(
        work, block, lanes, f_own, f_all, u_own, u_all, mx, out, counts, greet, first_halo, halo, max_copies, max_result
    )
    tiles = 22 * ROWS
    group = max((3 * by - 2) * 4, (3 * by - 2) * 2 + 12, 36)
    pl.run_scoped(
        body,
        pltpu.VMEM((bx * by * bz, 27, lanes, lanes), bf16),
        pltpu.VMEM((sides, lanes, tiles), bf16),
        pltpu.VMEM((bx * by, bz // 2, 3, tiles, 2 * lanes), bf16),
        pltpu.VMEM((group, lanes, 2 * lanes), bf16),
        pltpu.VMEM((group, lanes, 2 * lanes), bf16),
        pltpu.VMEM((sides, 3, 4 * ROWS, lanes), bf16),
        pltpu.VMEM((sides, 3, 2 * ROWS, lanes), bf16),
        pltpu.VMEM((sides, 2, ROWS, lanes), f32),
        pltpu.VMEM((bx * by, ROWS, lanes), f32),
        pltpu.VMEM((bx * by, 2, ROWS, lanes), f32),
    )


def work(block, lanes, f_own, f_all, u_own, u_all, mx, out, counts, greet, first_halo, halo, max_copies, max_result,
         k_all, bt, at, buf_a, buf_b, w0_all, w_all, vol, acc, sums):
    bx, by, bz = block
    nx, ny = bx + 2, by + 2
    row = lax.broadcasted_iota(jnp.int32, (ROWS, lanes), 0)
    inside = (row >= 1) & (row <= bz)
    known = row <= bz + 1
    last = ROWS - 1

    def start(copies):
        for c in copies:
            c.start()

    def wait(copies):
        for c in copies:
            c.wait()

    def centred(px, py, pz, x, y):
        cx = jnp.asarray(x, jnp.int32).astype(f32) - (0.5 * (bx + 1) + 0.5)
        cy = jnp.asarray(y, jnp.int32).astype(f32) - (0.5 * (by + 1) + 0.5)
        cz = row.astype(f32) - (0.5 * (bz + 1) + 0.5)
        px, py, pz = px + cx, py + cy, pz + cz
        return (px, py, pz), px * px + py * py + pz * pz

    def source(col, x, y, tile_of):
        pos, norm = centred(tile_of(0), tile_of(1), tile_of(2), x, y)
        parts = []
        for p in pos:
            hi, mid, lo = split3(p)
            parts += [hi, mid, hi, mid, lo, hi]
        parts += [jnp.where(row == last, 1.0, part) for part in split3(norm)]
        parts.append(jnp.zeros((ROWS, lanes), f32))
        stack = jnp.concatenate(parts, axis=0).astype(bf16)
        bt[col] = stack.T

    def own_sources(x, carry):
        for y in range(by):
            source((x + 1) * ny + y + 1, x + 1, y + 1, lambda k, y=y: f_own[k, x, y])
        return carry

    lax.fori_loop(0, bx, own_sources, 0)

    def targets(x, carry):
        for y in range(by):
            pos, norm = centred(f_own[0, x, y], f_own[1, x, y], f_own[2, x, y], x + 1, y + 1)
            coefs = [split3(-2.0 * p) for p in pos]
            norms = split3(norm)
            moved = [[[pltpu.roll(part, ez % ROWS, 0) if ez else part for part in c] for c in coefs] for ez in (-1, 0, 1)]
            for zp in range(bz // 2):
                for ez in (-1, 0, 1):
                    halves = []
                    for t in (2 * zp + 1, 2 * zp + 2):
                        here = row == t + ez
                        parts = []
                        for c in moved[ez + 1]:
                            hi, mid, lo = [jnp.where(here, part, 0.0) for part in c]
                            parts += [hi, hi, mid, mid, hi, lo]
                        for part in norms:
                            at_last = pltpu.roll(part, last - t, 0)
                            parts.append(jnp.where(here, 1.0, jnp.where(row == last, at_last, 0.0)))
                        parts.append(jnp.zeros((ROWS, lanes), f32))
                        halves.append(jnp.concatenate(parts, axis=0).astype(bf16))
                    at[x * by + y, zp, ez + 1] = jnp.concatenate(halves, axis=1)
        return carry

    lax.fori_loop(0, bx, targets, 0)
    greet()

    def unit(x, y, cx, cy, zp, ez):
        return dict(t=x * by + y, c=(cx + 1) * ny + cy + 1, zp=zp, ez=ez, slot=((cx - x + 1) * 3 + cy - y + 1) * 3 + ez + 1)

    def gemm(buf, units):
        for i, u in enumerate(units):
            dist_sq = jnp.dot(bt[u["c"]], at[u["t"], u["zp"], u["ez"] + 1], preferred_element_type=f32)
            buf[i] = dist_sq.astype(bf16)

    def spread(buf, units):
        for i, u in enumerate(units):
            for half in range(2):
                dist_sq = jnp.maximum(buf[i, :, half * lanes : (half + 1) * lanes], jnp.array(1e-12, bf16))
                near = jnp.maximum(1.0 - dist_sq * lax.rsqrt(dist_sq), jnp.zeros((), bf16))
                k_all[u["t"] * bz + 2 * u["zp"] + half, u["slot"]] = near * near * near

    def run(now, other, groups, units):
        def step(i, carry):
            gemm(other, units(2 * i + 1))
            spread(now, units(2 * i))
            gemm(now, units(2 * i + 2))
            spread(other, units(2 * i + 1))
            return carry

        lax.fori_loop(0, (groups - 1) // 2, step, 0)
        if groups % 2 == 0:
            gemm(other, units(groups - 1))
            spread(now, units(groups - 2))
            now, other = other, now
        return now, other

    y_pairs = [(y, cy) for y in range(by) for cy in (y - 1, y, y + 1) if 0 <= cy < by]
    y_rims = [(0, -1), (by - 1, by)]
    n_pairs = 3 * bx - 2

    def x_pair(k):
        x = (k + 1) // 3
        return x, k - 2 * x

    def own_units(k):
        x, cx = x_pair(k)
        return [unit(x, y, cx, cy, zp, ez - zp) for zp in (0, 1) for y, cy in y_pairs for ez in (0, 1)]

    def rim_units(k):
        x, cx = x_pair(k)
        return [unit(x, y, cx, cy, zp, 2 * zp - 1) for zp in (0, 1) for y, cy in y_pairs] + [
            unit(x, y, cx, cy, zp, ez) for zp in (0, 1) for y, cy in y_rims for ez in (-1, 0, 1)
        ]

    def far_units(y):
        return [
            unit(x, y, cx, y + ey, zp, ez)
            for x, cx in ((0, -1), (bx - 1, bx))
            for zp in (0, 1)
            for ey in (-1, 0, 1)
            for ez in (-1, 0, 1)
        ]

    gemm(buf_a, own_units(0))
    now, other = run(buf_a, buf_b, n_pairs, own_units)
    wait(first_halo)

    def all_sources(x, carry):
        for y in range(ny):
            source(x * ny + y, x, y, lambda k, y=y: jnp.where(known, f_all[k, x, y], 0.0))
        return carry

    lax.fori_loop(0, nx, all_sources, 0)

    def shifted(ref, col, pairs):
        for ez in (-1, 0, 1):
            his, los = [], []
            for first, second in pairs:
                both = jnp.where(
                    row < bz, pltpu.roll(first, (-1 - ez) % ROWS, 0), pltpu.roll(second, (bz - 1 - ez) % ROWS, 0)
                )
                hi, lo = split2(both)
                his.append(hi)
                los.append(lo)
            ref[col, ez + 1] = jnp.concatenate(his + los, axis=0).astype(bf16)

    def apart(tile):
        return pltpu.roll(tile, 1, 0), pltpu.roll(tile, (1 - bz) % ROWS, 0)

    def weigh_first(x, carry):
        for y in range(ny):
            col = x * ny + y
            v, u = f_all[3, x, y], f_all[HEAT, x, y]
            vc = v * (u * u * jnp.sqrt(u))
            vol[col, 0] = v
            vol[col, 1] = vc
            shifted(w0_all, col, [(v, vc), (v * u, vc * u)])
        return carry

    lax.fori_loop(0, nx, weigh_first, 0)
    gemm(other, rim_units(0))
    spread(now, own_units(n_pairs - 1))
    now, other = run(other, now, n_pairs, rim_units)
    gemm(other, far_units(0))
    spread(now, rim_units(n_pairs - 1))
    now, other = run(other, now, by, far_units)
    spread(now, far_units(by - 1))

    same = lax.broadcasted_iota(jnp.int32, (lanes, lanes), 0) == lax.broadcasted_iota(jnp.int32, (lanes, lanes), 1)
    same = same.astype(f32).astype(bf16)

    def itself(t, carry):
        for z in range(bz):
            k_all[t * bz + z, 13] = jnp.maximum(k_all[t * bz + z, 13], same)
        return carry

    lax.fori_loop(0, bx * by, itself, 0)

    def reduce(w_ref, kinds, x, y, lists):
        total = jnp.zeros((kinds * ROWS, lanes), f32)
        wide = lax.broadcasted_iota(jnp.int32, (kinds * ROWS, lanes), 0) % bz
        for z in range(bz):
            items = [(cx, cy, ez) for cx, cy, ez in lists[z]]
            if not items:
                continue
            w = jnp.concatenate([w_ref[(cx + 1) * ny + cy + 1, ez + 1] for cx, cy, ez in items], axis=1)
            k = jnp.concatenate(
                [k_all[(x * by + y) * bz + z, ((cx - x + 1) * 3 + cy - y + 1) * 3 + ez + 1] for cx, cy, ez in items], axis=0
            )
            o = jnp.dot(w, k, preferred_element_type=f32)
            o = o[: kinds * ROWS] + o[kinds * ROWS :]
            total = jnp.where(wide == z, o, total)
        return total

    def flow_of(s_vu, s_vcu, s_v, s_vc, u, c):
        return c * (s_vu - u * s_v) + (s_vcu - u * s_vc)

    def heat_power(u):
        return u * u * jnp.sqrt(u)

    def emit(step, x, y, flow):
        u_own[step, x, y] = flow
        u_all[step, x + 1, y + 1, 1 : bz + 1] = flow[1 : bz + 1]

    every = [[(ex, ey, ez) for ex in (-1, 0, 1) for ey in (-1, 0, 1) for ez in (-1, 0, 1)] for z in range(bz)]

    def apply_first(x, largest):
        for y in range(by):
            lists = [[(x + ex, y + ey, ez) for ex, ey, ez in every[z]] for z in range(bz)]
            o = reduce(w0_all, 2, x, y, lists)
            s_v, s_vc = apart(o[:ROWS])
            s_vu, s_vcu = apart(o[ROWS:])
            u = f_own[HEAT, x, y]
            c = heat_power(u)
            sums[x * by + y, 0] = s_v
            sums[x * by + y, 1] = s_vc
            emit(0, x, y, jnp.where(inside, flow_of(s_vu, s_vcu, s_v, s_vc, u, c), 0.0))
            rows = c * s_v + s_vc
            lane = lax.broadcasted_iota(jnp.int32, (ROWS, lanes), 1)
            filled = jnp.zeros((ROWS, lanes), jnp.int32)
            for z in range(bz):
                filled = jnp.where(row == z + 1, counts[x, y, z], filled)
            largest = jnp.maximum(largest, jnp.where(inside & (lane < filled), rows, 0.0))
        return largest

    mx[0] = lax.fori_loop(0, bx, apply_first, jnp.zeros((ROWS, lanes), f32))
    halo1 = halo(0)
    max0 = max_copies(0)
    start(halo1)
    start(max0)

    def weigh(step, x, y, u):
        col = (x + 1) * ny + y + 1
        shifted(w_all, col, [(vol[col, 0] * u, vol[col, 1] * u)])

    own_cols = [(x, y) for x in range(bx) for y in range(by)]
    face_cols = [(x, y) for x in (-1, bx) for y in range(by)] + [(x, y) for x in range(bx) for y in (-1, by)]
    edge_cols = [(x, y) for x in (-1, bx) for y in (-1, by)]

    def outside(x, y, z):
        return sum(not 0 <= i < n for i, n in zip((x, y, z), block))

    def blocks(x, y, wanted):
        return [
            [(x + ex, y + ey, ez) for ex, ey, ez in every[z] if outside(x + ex, y + ey, z + ez) in wanted] for z in range(bz)
        ]

    def apply_own(step):
        for x, y in own_cols:
            weigh(step, x, y, u_own[step, x, y])
        for x, y in own_cols:
            acc[x * by + y] = reduce(w_all, 1, x, y, blocks(x, y, (0,)))

    def apply_faces(step, copies):
        wait([c for c, d in zip(copies, DIRS) if sum(map(abs, d)) == 1])
        for x, y in own_cols:
            weigh(step, x, y, u_all[step, x + 1, y + 1])
        for x, y in face_cols:
            weigh(step, x, y, padded(u_all[step, x + 1, y + 1, 1 : bz + 1]))
        for x, y in own_cols:
            acc[x * by + y] += reduce(w_all, 1, x, y, blocks(x, y, (1,)))

    def apply_rest(step, copies, emit_flow):
        wait([c for c, d in zip(copies, DIRS) if sum(map(abs, d)) > 1])
        for x, y in face_cols + edge_cols:
            weigh(step, x, y, u_all[step, x + 1, y + 1])
        for x, y in own_cols:
            t = x * by + y
            s_vu, s_vcu = apart(acc[t] + reduce(w_all, 1, x, y, blocks(x, y, (2, 3))))
            u = u_own[step, x, y]
            emit_flow(x, y, flow_of(s_vu, s_vcu, sums[t, 0], sums[t, 1], u, heat_power(f_own[HEAT, x, y])))

    apply_own(0)
    wait(max0)
    mx[1] = max_result(0)
    max1 = max_copies(1)
    start(max1)
    apply_faces(0, halo1)
    apply_rest(0, halo1, lambda x, y, flow: emit(1, x, y, jnp.where(inside, flow, 0.0)))
    halo2 = halo(1)
    start(halo2)
    wait(max1)
    mx[2] = max_result(1)
    max2 = max_copies(2)
    start(max2)
    apply_own(1)
    apply_faces(1, halo2)
    wait(max2)
    top = jnp.max(jnp.max(max_result(2), axis=1, keepdims=True), axis=0, keepdims=True)
    step = 2.0 / top

    def finish(x, y, f2):
        f0, f1 = u_own[0, x, y], u_own[1, x, y]
        d_first = 2.0 / 15.0 * step * f0
        l_first = f0 + 2.0 / 15.0 * step * f1
        l_l_first = f1 + 2.0 / 15.0 * step * f2
        d_second = 1.5 * d_first + 0.6 * step * l_first - 0.4 * step * f0
        l_second = 1.5 * l_first - 0.5 * f0 + 0.6 * step * l_l_first - 0.4 * step * f1
        rise = 25.0 / 12.0 * d_second - 5.0 / 6.0 * d_first + 5.0 / 6.0 * step * l_second - 5.0 / 9.0 * step * f0
        out[x, y] = rise[1 : bz + 1]

    apply_rest(1, halo2, finish)


def local(relative_placements, mass_per_density, opening_heat_level, bin_fill_counts):
    lanes = opening_heat_level.shape[-1]
    block = opening_heat_level.shape[:3]
    dims = tuple(lax.axis_size(a) for a in AXES)
    bx, by, bz = block
    assert bz == 4
    vmem = pl.BlockSpec(memory_space=pltpu.VMEM)
    dma = pltpu.SemaphoreType.DMA
    n_dirs = len(DIRS)
    rise = pl.pallas_call(
        functools.partial(kernel, dims, block),
        out_shape=jax.ShapeDtypeStruct(block + (lanes,), f32),
        in_specs=[pl.BlockSpec(memory_space=pltpu.SMEM), vmem, vmem, vmem],
        out_specs=vmem,
        scratch_shapes=[
            pltpu.VMEM((HEAT + 1, bx, by, ROWS, lanes), f32),
            pltpu.VMEM((HEAT + 1, bx + 2, by + 2, ROWS, lanes), f32),
            pltpu.VMEM((2, bx, by, ROWS, lanes), f32),
            pltpu.VMEM((2, bx + 2, by + 2, ROWS, lanes), f32),
            pltpu.VMEM((3, ROWS, lanes), f32),
            pltpu.VMEM((sum(dims), ROWS, lanes), f32),
            dma((n_dirs,)),
            dma((n_dirs,)),
            dma((2, n_dirs)),
            dma((2, n_dirs)),
            dma((sum(dims),)),
            dma((sum(dims),)),
        ],
        compiler_params=pltpu.CompilerParams(
            collective_id=0, has_side_effects=True, vmem_limit_bytes=60 * 1024 * 1024
        ),
    )(bin_fill_counts, relative_placements, mass_per_density, opening_heat_level)
    return opening_heat_level + rise


def solution(mesh):
    in_specs = (
        P(None, "gx", "gy", "gz", None),
        P("gx", "gy", "gz", None),
        P("gx", "gy", "gz", None),
        P("gx", "gy", "gz"),
    )
    out_specs = P("gx", "gy", "gz", None)
    return jax.shard_map(local, mesh=mesh, in_specs=in_specs, out_specs=out_specs, check_vma=False)
```

```python
import functools
import itertools
import jax
import jax.numpy as jnp
from jax import lax
from jax.experimental import pallas as pl
from jax.experimental.pallas import tpu as pltpu
from jax.sharding import PartitionSpec as P

AXES = ("gx", "gy", "gz")
MESH = pl.DeviceIdType.MESH
f32, bf16 = jnp.float32, jnp.bfloat16
DIRS = [d for d in itertools.product((-1, 0, 1), repeat=3) if d != (0, 0, 0)]
ROWS = 8
HEAT = 4


def split3(tile):
    hi = tile.astype(bf16).astype(f32)
    rest = tile - hi
    mid = rest.astype(bf16).astype(f32)
    return hi, mid, rest - mid


def split2(tile):
    hi = tile.astype(bf16).astype(f32)
    return hi, tile - hi


def padded(tile):
    lanes = tile.shape[-1]
    pad = [jnp.zeros((1, lanes), f32), tile, jnp.zeros((ROWS - 1 - tile.shape[0], lanes), f32)]
    return jnp.concatenate(pad, axis=0)


def kernel(dims, block, counts, offsets, mass, heat, out, f_own, f_all, u_own, u_all, mx, mx_parts, fsend, frecv, usend, urecv, msend, mrecv):
    bx, by, bz = block
    lanes = heat.shape[-1]
    me = [lax.axis_index(a) for a in AXES]

    def neighbour(d):
        return tuple(lax.rem(me[k] + (d[k] + dims[k]), dims[k]) if d[k] else me[k] for k in range(3))

    hops = [
        [(h, 0, 0) for h in range(1, dims[0])],
        [(0, h, i) for h in range(dims[1]) for i in range(dims[2]) if (h, i) != (0, 0)],
    ]

    def peer(hop):
        return tuple(lax.rem(me[k] + hop[k], dims[k]) if hop[k] else me[k] for k in range(3))

    barrier = pltpu.get_barrier_semaphore()
    count = 0
    for d in DIRS:
        pl.semaphore_signal(barrier, inc=1, device_id=neighbour(d), device_id_type=MESH)
        count += 1
    for hop in hops[0] + hops[1]:
        pl.semaphore_signal(barrier, inc=1, device_id=peer(hop), device_id_type=MESH)
        count += 1

    row = lax.broadcasted_iota(jnp.int32, (ROWS, lanes), 0)
    lane = lax.broadcasted_iota(jnp.int32, (ROWS, lanes), 1)
    zero = jnp.zeros((ROWS, lanes), f32)

    def load_own(x, carry):
        for y in range(by):
            filled = jnp.zeros((ROWS, lanes), jnp.int32)
            for z in range(bz):
                filled = jnp.where(row == z + 1, counts[x, y, z], filled)
            parts = [offsets[0, x, y], offsets[1, x, y], offsets[2, x, y], mass[x, y], heat[x, y]]
            for k, part in enumerate(parts):
                tile = padded(part)
                if k == 3:
                    tile = jnp.where(lane < filled, tile, 0.0)
                f_own[k, x, y] = tile
                f_all[k, x + 1, y + 1, 1 : bz + 1] = tile[1 : bz + 1]
        return carry

    lax.fori_loop(0, bx, load_own, 0)

    def piece(d):
        src, dst = [], []
        for k in range(3):
            n, base = block[k], 1 if k == 2 else 0
            if d[k] == 0:
                src.append(pl.ds(base, n))
                dst.append(pl.ds(1, n))
            elif d[k] == 1:
                src.append(pl.ds(base + n - 1, 1))
                dst.append(pl.ds(0, 1))
            else:
                src.append(pl.ds(base, 1))
                dst.append(pl.ds(n + 1, 1))
        return tuple(src), tuple(dst)

    def halo_copies(src_ref, lead_src, dst_ref, lead_dst, ssem, rsem):
        copies = []
        for i, d in enumerate(DIRS):
            src, dst = piece(d)
            copies.append(
                pltpu.make_async_remote_copy(
                    src_ref=src_ref.at[(lead_src,) + src],
                    dst_ref=dst_ref.at[(lead_dst,) + dst],
                    send_sem=ssem.at[i],
                    recv_sem=rsem.at[i],
                    device_id=neighbour(d),
                    device_id_type=MESH,
                )
            )
        return copies

    def max_copies(phase):
        begin = phase * len(hops[0])
        return [
            pltpu.make_async_remote_copy(
                src_ref=mx.at[phase],
                dst_ref=mx_parts.at[begin + i],
                send_sem=msend.at[begin + i],
                recv_sem=mrecv.at[begin + i],
                device_id=peer(hop),
                device_id_type=MESH,
            )
            for i, hop in enumerate(hops[phase])
        ]

    def max_result(phase):
        begin = phase * len(hops[0])
        total = mx[phase]
        for i in range(len(hops[phase])):
            total = jnp.maximum(total, mx_parts[begin + i])
        return total

    fields = pl.ds(0, f_own.shape[0])
    first_halo = halo_copies(f_own, fields, f_all, fields, fsend, frecv)

    def greet():
        pl.semaphore_wait(barrier, count)
        for c in first_halo:
            c.start()

    def halo(step):
        return halo_copies(u_own, step, u_all, step, usend.at[step], urecv.at[step])

    sides = (bx + 2) * (by + 2)
    body = functools.partial(
        work, block, lanes, f_own, f_all, u_own, u_all, mx, out, counts, greet, first_halo, halo, max_copies, max_result
    )
    tiles = 22 * ROWS
    group = max((3 * by - 2) * 4, (3 * by - 2) * 2 + 12, 36)
    pl.run_scoped(
        body,
        pltpu.VMEM((bx * by * bz, 27, lanes, lanes), bf16),
        pltpu.VMEM((sides, lanes, tiles), bf16),
        pltpu.VMEM((bx * by, bz // 2, 3, tiles, 2 * lanes), bf16),
        pltpu.VMEM((group, lanes, 2 * lanes), bf16),
        pltpu.VMEM((group, lanes, 2 * lanes), bf16),
        pltpu.VMEM((sides, 3, 4 * ROWS, lanes), bf16),
        pltpu.VMEM((sides, 3, 2 * ROWS, lanes), bf16),
        pltpu.VMEM((sides, 2, ROWS, lanes), f32),
        pltpu.VMEM((bx * by, ROWS, lanes), f32),
        pltpu.VMEM((bx * by, 2, ROWS, lanes), f32),
    )


def work(block, lanes, f_own, f_all, u_own, u_all, mx, out, counts, greet, first_halo, halo, max_copies, max_result,
         k_all, bt, at, buf_a, buf_b, w0_all, w_all, vol, acc, sums):
    bx, by, bz = block
    nx, ny = bx + 2, by + 2
    row = lax.broadcasted_iota(jnp.int32, (ROWS, lanes), 0)
    inside = (row >= 1) & (row <= bz)
    known = row <= bz + 1
    last = ROWS - 1

    def start(copies):
        for c in copies:
            c.start()

    def wait(copies):
        for c in copies:
            c.wait()

    def nearest_first(copies):
        return [copies[i] for i in sorted(range(len(DIRS)), key=lambda i: sum(map(abs, DIRS[i])))]

    def centred(px, py, pz, x, y):
        cx = jnp.asarray(x, jnp.int32).astype(f32) - (0.5 * (bx + 1) + 0.5)
        cy = jnp.asarray(y, jnp.int32).astype(f32) - (0.5 * (by + 1) + 0.5)
        cz = row.astype(f32) - (0.5 * (bz + 1) + 0.5)
        px, py, pz = px + cx, py + cy, pz + cz
        return (px, py, pz), px * px + py * py + pz * pz

    def source(col, x, y, tile_of):
        pos, norm = centred(tile_of(0), tile_of(1), tile_of(2), x, y)
        parts = []
        for p in pos:
            hi, mid, lo = split3(p)
            parts += [hi, mid, hi, mid, lo, hi]
        parts += [jnp.where(row == last, 1.0, part) for part in split3(norm)]
        parts.append(jnp.zeros((ROWS, lanes), f32))
        stack = jnp.concatenate(parts, axis=0).astype(bf16)
        bt[col] = stack.T

    def own_sources(x, carry):
        for y in range(by):
            source((x + 1) * ny + y + 1, x + 1, y + 1, lambda k, y=y: f_own[k, x, y])
        return carry

    lax.fori_loop(0, bx, own_sources, 0)

    def targets(x, carry):
        for y in range(by):
            pos, norm = centred(f_own[0, x, y], f_own[1, x, y], f_own[2, x, y], x + 1, y + 1)
            coefs = [split3(-2.0 * p) for p in pos]
            norms = split3(norm)
            moved = [[[pltpu.roll(part, ez % ROWS, 0) if ez else part for part in c] for c in coefs] for ez in (-1, 0, 1)]
            for zp in range(bz // 2):
                for ez in (-1, 0, 1):
                    halves = []
                    for t in (2 * zp + 1, 2 * zp + 2):
                        here = row == t + ez
                        parts = []
                        for c in moved[ez + 1]:
                            hi, mid, lo = [jnp.where(here, part, 0.0) for part in c]
                            parts += [hi, hi, mid, mid, hi, lo]
                        for part in norms:
                            at_last = pltpu.roll(part, last - t, 0)
                            parts.append(jnp.where(here, 1.0, jnp.where(row == last, at_last, 0.0)))
                        parts.append(jnp.zeros((ROWS, lanes), f32))
                        halves.append(jnp.concatenate(parts, axis=0).astype(bf16))
                    at[x * by + y, zp, ez + 1] = jnp.concatenate(halves, axis=1)
        return carry

    lax.fori_loop(0, bx, targets, 0)
    greet()

    def unit(x, y, cx, cy, zp, ez):
        return dict(t=x * by + y, c=(cx + 1) * ny + cy + 1, zp=zp, ez=ez, slot=((cx - x + 1) * 3 + cy - y + 1) * 3 + ez + 1)

    def gemm(buf, units):
        for i, u in enumerate(units):
            dist_sq = jnp.dot(bt[u["c"]], at[u["t"], u["zp"], u["ez"] + 1], preferred_element_type=f32)
            buf[i] = jnp.maximum(dist_sq.astype(bf16), jnp.array(1e-12, bf16))

    def spread(buf, units):
        for i, u in enumerate(units):
            for half in range(2):
                dist_sq = buf[i, :, half * lanes : (half + 1) * lanes]
                near = jnp.maximum(1.0 - dist_sq * lax.rsqrt(dist_sq), jnp.zeros((), bf16))
                k_all[u["t"] * bz + 2 * u["zp"] + half, u["slot"]] = near * near * near

    def run(now, other, groups, units):
        def step(i, carry):
            gemm(other, units(2 * i + 1))
            spread(now, units(2 * i))
            gemm(now, units(2 * i + 2))
            spread(other, units(2 * i + 1))
            return carry

        lax.fori_loop(0, (groups - 1) // 2, step, 0)
        if groups % 2 == 0:
            gemm(other, units(groups - 1))
            spread(now, units(groups - 2))
            now, other = other, now
        return now, other

    y_pairs = [(y, cy) for y in range(by) for cy in (y - 1, y, y + 1) if 0 <= cy < by]
    y_rims = [(0, -1), (by - 1, by)]
    n_pairs = 3 * bx - 2

    def x_pair(k):
        x = (k + 1) // 3
        return x, k - 2 * x

    def own_units(k):
        x, cx = x_pair(k)
        return [unit(x, y, cx, cy, zp, ez - zp) for zp in (0, 1) for y, cy in y_pairs for ez in (0, 1)]

    def rim_units(k):
        x, cx = x_pair(k)
        return [unit(x, y, cx, cy, zp, 2 * zp - 1) for zp in (0, 1) for y, cy in y_pairs] + [
            unit(x, y, cx, cy, zp, ez) for zp in (0, 1) for y, cy in y_rims for ez in (-1, 0, 1)
        ]

    def far_units(y):
        return [
            unit(x, y, cx, y + ey, zp, ez)
            for x, cx in ((0, -1), (bx - 1, bx))
            for zp in (0, 1)
            for ey in (-1, 0, 1)
            for ez in (-1, 0, 1)
        ]

    gemm(buf_a, own_units(0))
    now, other = run(buf_a, buf_b, n_pairs, own_units)
    wait(first_halo)

    def all_sources(x, carry):
        for y in range(ny):
            source(x * ny + y, x, y, lambda k, y=y: jnp.where(known, f_all[k, x, y], 0.0))
        return carry

    lax.fori_loop(0, nx, all_sources, 0)

    def shifted(ref, col, pairs):
        for ez in (-1, 0, 1):
            his, los = [], []
            for first, second in pairs:
                both = jnp.where(
                    row < bz, pltpu.roll(first, (-1 - ez) % ROWS, 0), pltpu.roll(second, (bz - 1 - ez) % ROWS, 0)
                )
                hi, lo = split2(both)
                his.append(hi)
                los.append(lo)
            ref[col, ez + 1] = jnp.concatenate(his + los, axis=0).astype(bf16)

    def apart(tile):
        return pltpu.roll(tile, 1, 0), pltpu.roll(tile, (1 - bz) % ROWS, 0)

    def weigh_first(x, carry):
        for y in range(ny):
            col = x * ny + y
            v, u = f_all[3, x, y], f_all[HEAT, x, y]
            vc = v * (u * u * jnp.sqrt(u))
            vol[col, 0] = v
            vol[col, 1] = vc
            shifted(w0_all, col, [(v, vc), (v * u, vc * u)])
        return carry

    lax.fori_loop(0, nx, weigh_first, 0)
    gemm(other, rim_units(0))
    spread(now, own_units(n_pairs - 1))
    now, other = run(other, now, n_pairs, rim_units)
    gemm(other, far_units(0))
    spread(now, rim_units(n_pairs - 1))
    now, other = run(other, now, by, far_units)
    spread(now, far_units(by - 1))

    same = lax.broadcasted_iota(jnp.int32, (lanes, lanes), 0) == lax.broadcasted_iota(jnp.int32, (lanes, lanes), 1)
    same = same.astype(f32).astype(bf16)

    def itself(t, carry):
        for z in range(bz):
            k_all[t * bz + z, 13] = jnp.maximum(k_all[t * bz + z, 13], same)
        return carry

    lax.fori_loop(0, bx * by, itself, 0)

    def reduce(w_ref, kinds, x, y, lists):
        total = jnp.zeros((kinds * ROWS, lanes), f32)
        wide = lax.broadcasted_iota(jnp.int32, (kinds * ROWS, lanes), 0) % bz
        for z in range(bz):
            items = [(cx, cy, ez) for cx, cy, ez in lists[z]]
            if not items:
                continue
            w = jnp.concatenate([w_ref[(cx + 1) * ny + cy + 1, ez + 1] for cx, cy, ez in items], axis=1)
            k = jnp.concatenate(
                [k_all[(x * by + y) * bz + z, ((cx - x + 1) * 3 + cy - y + 1) * 3 + ez + 1] for cx, cy, ez in items], axis=0
            )
            o = jnp.dot(w, k, preferred_element_type=f32)
            o = o[: kinds * ROWS] + o[kinds * ROWS :]
            total = jnp.where(wide == z, o, total)
        return total

    def flow_of(s_vu, s_vcu, s_v, s_vc, u, c):
        return c * (s_vu - u * s_v) + (s_vcu - u * s_vc)

    def heat_power(u):
        return u * u * jnp.sqrt(u)

    def emit(step, x, y, flow):
        u_own[step, x, y] = flow
        u_all[step, x + 1, y + 1, 1 : bz + 1] = flow[1 : bz + 1]

    every = [[(ex, ey, ez) for ex in (-1, 0, 1) for ey in (-1, 0, 1) for ez in (-1, 0, 1)] for z in range(bz)]

    def apply_first(x, largest):
        for y in range(by):
            lists = [[(x + ex, y + ey, ez) for ex, ey, ez in every[z]] for z in range(bz)]
            o = reduce(w0_all, 2, x, y, lists)
            s_v, s_vc = apart(o[:ROWS])
            s_vu, s_vcu = apart(o[ROWS:])
            u = f_own[HEAT, x, y]
            c = heat_power(u)
            sums[x * by + y, 0] = s_v
            sums[x * by + y, 1] = s_vc
            emit(0, x, y, jnp.where(inside, flow_of(s_vu, s_vcu, s_v, s_vc, u, c), 0.0))
            rows = c * s_v + s_vc
            lane = lax.broadcasted_iota(jnp.int32, (ROWS, lanes), 1)
            filled = jnp.zeros((ROWS, lanes), jnp.int32)
            for z in range(bz):
                filled = jnp.where(row == z + 1, counts[x, y, z], filled)
            largest = jnp.maximum(largest, jnp.where(inside & (lane < filled), rows, 0.0))
        return largest

    mx[0] = lax.fori_loop(0, bx, apply_first, jnp.zeros((ROWS, lanes), f32))
    halo1 = halo(0)
    max0 = max_copies(0)
    start(nearest_first(halo1))
    start(max0)

    def weigh(step, x, y, u):
        col = (x + 1) * ny + y + 1
        shifted(w_all, col, [(vol[col, 0] * u, vol[col, 1] * u)])

    own_cols = [(x, y) for x in range(bx) for y in range(by)]
    face_cols = [(x, y) for x in (-1, bx) for y in range(by)] + [(x, y) for x in range(bx) for y in (-1, by)]
    edge_cols = [(x, y) for x in (-1, bx) for y in (-1, by)]

    def outside(x, y, z):
        return sum(not 0 <= i < n for i, n in zip((x, y, z), block))

    def blocks(x, y, wanted):
        return [
            [(x + ex, y + ey, ez) for ex, ey, ez in every[z] if outside(x + ex, y + ey, z + ez) in wanted] for z in range(bz)
        ]

    def apply_own(step):
        for x, y in own_cols:
            weigh(step, x, y, u_own[step, x, y])
        for x, y in own_cols:
            acc[x * by + y] = reduce(w_all, 1, x, y, blocks(x, y, (0,)))

    def apply_faces(step, copies):
        wait([c for c, d in zip(copies, DIRS) if sum(map(abs, d)) == 1])
        for x, y in own_cols:
            weigh(step, x, y, u_all[step, x + 1, y + 1])
        for x, y in face_cols:
            weigh(step, x, y, padded(u_all[step, x + 1, y + 1, 1 : bz + 1]))
        for x, y in own_cols:
            acc[x * by + y] += reduce(w_all, 1, x, y, blocks(x, y, (1,)))

    def apply_rest(step, copies, emit_flow):
        wait([c for c, d in zip(copies, DIRS) if sum(map(abs, d)) > 1])
        for x, y in face_cols + edge_cols:
            weigh(step, x, y, u_all[step, x + 1, y + 1])
        for x, y in own_cols:
            t = x * by + y
            s_vu, s_vcu = apart(acc[t] + reduce(w_all, 1, x, y, blocks(x, y, (2, 3))))
            u = u_own[step, x, y]
            emit_flow(x, y, flow_of(s_vu, s_vcu, sums[t, 0], sums[t, 1], u, heat_power(f_own[HEAT, x, y])))

    apply_own(0)
    apply_faces(0, halo1)
    apply_rest(0, halo1, lambda x, y, flow: emit(1, x, y, jnp.where(inside, flow, 0.0)))
    halo2 = halo(1)
    start(nearest_first(halo2))
    wait(max0)
    mx[1] = max_result(0)
    max1 = max_copies(1)
    start(max1)
    apply_own(1)
    apply_faces(1, halo2)
    wait(max1)
    top = jnp.max(jnp.max(max_result(1), axis=1, keepdims=True), axis=0, keepdims=True)
    step = 2.0 / top

    def finish(x, y, f2):
        f0, f1 = u_own[0, x, y], u_own[1, x, y]
        d_first = 2.0 / 15.0 * step * f0
        l_first = f0 + 2.0 / 15.0 * step * f1
        l_l_first = f1 + 2.0 / 15.0 * step * f2
        d_second = 1.5 * d_first + 0.6 * step * l_first - 0.4 * step * f0
        l_second = 1.5 * l_first - 0.5 * f0 + 0.6 * step * l_l_first - 0.4 * step * f1
        rise = 25.0 / 12.0 * d_second - 5.0 / 6.0 * d_first + 5.0 / 6.0 * step * l_second - 5.0 / 9.0 * step * f0
        out[x, y] = rise[1 : bz + 1]

    apply_rest(1, halo2, finish)


def local(relative_placements, mass_per_density, opening_heat_level, bin_fill_counts):
    lanes = opening_heat_level.shape[-1]
    block = opening_heat_level.shape[:3]
    dims = tuple(lax.axis_size(a) for a in AXES)
    bx, by, bz = block
    assert bz == 4
    vmem = pl.BlockSpec(memory_space=pltpu.VMEM)
    dma = pltpu.SemaphoreType.DMA
    n_dirs = len(DIRS)
    n_peers = dims[0] - 1 + dims[1] * dims[2] - 1
    rise = pl.pallas_call(
        functools.partial(kernel, dims, block),
        out_shape=jax.ShapeDtypeStruct(block + (lanes,), f32),
        in_specs=[pl.BlockSpec(memory_space=pltpu.SMEM), vmem, vmem, vmem],
        out_specs=vmem,
        scratch_shapes=[
            pltpu.VMEM((HEAT + 1, bx, by, ROWS, lanes), f32),
            pltpu.VMEM((HEAT + 1, bx + 2, by + 2, ROWS, lanes), f32),
            pltpu.VMEM((2, bx, by, ROWS, lanes), f32),
            pltpu.VMEM((2, bx + 2, by + 2, ROWS, lanes), f32),
            pltpu.VMEM((2, ROWS, lanes), f32),
            pltpu.VMEM((n_peers, ROWS, lanes), f32),
            dma((n_dirs,)),
            dma((n_dirs,)),
            dma((2, n_dirs)),
            dma((2, n_dirs)),
            dma((n_peers,)),
            dma((n_peers,)),
        ],
        compiler_params=pltpu.CompilerParams(
            collective_id=0, has_side_effects=True, vmem_limit_bytes=60 * 1024 * 1024
        ),
    )(bin_fill_counts, relative_placements, mass_per_density, opening_heat_level)
    return opening_heat_level + rise


def solution(mesh):
    in_specs = (
        P(None, "gx", "gy", "gz", None),
        P("gx", "gy", "gz", None),
        P("gx", "gy", "gz", None),
        P("gx", "gy", "gz"),
    )
    out_specs = P("gx", "gy", "gz", None)
    return jax.shard_map(local, mesh=mesh, in_specs=in_specs, out_specs=out_specs, check_vma=False)
```

```python
import functools
import itertools
import jax
import jax.numpy as jnp
from jax import lax
from jax.experimental import pallas as pl
from jax.experimental.pallas import tpu as pltpu
from jax.sharding import PartitionSpec as P

AXES = ("gx", "gy", "gz")
MESH = pl.DeviceIdType.MESH
f32, bf16 = jnp.float32, jnp.bfloat16
DIRS = [d for d in itertools.product((-1, 0, 1), repeat=3) if d != (0, 0, 0)]
ROWS = 8
HEAT = 4


def split3(tile):
    hi = tile.astype(bf16).astype(f32)
    rest = tile - hi
    mid = rest.astype(bf16).astype(f32)
    return hi, mid, rest - mid


def split2(tile):
    hi = tile.astype(bf16).astype(f32)
    return hi, tile - hi


def padded(tile):
    lanes = tile.shape[-1]
    pad = [jnp.zeros((1, lanes), f32), tile, jnp.zeros((ROWS - 1 - tile.shape[0], lanes), f32)]
    return jnp.concatenate(pad, axis=0)


def kernel(dims, block, counts, offsets, mass, heat, out, f_own, f_all, u_own, u_all, mx, mx_parts, fsend, frecv, usend, urecv, msend, mrecv):
    bx, by, bz = block
    lanes = heat.shape[-1]
    me = [lax.axis_index(a) for a in AXES]

    def neighbour(d):
        return tuple(lax.rem(me[k] + (d[k] + dims[k]), dims[k]) if d[k] else me[k] for k in range(3))

    hops = [
        [(h, 0, 0) for h in range(1, dims[0])],
        [(0, h, i) for h in range(dims[1]) for i in range(dims[2]) if (h, i) != (0, 0)],
    ]

    def peer(hop):
        return tuple(lax.rem(me[k] + hop[k], dims[k]) if hop[k] else me[k] for k in range(3))

    barrier = pltpu.get_barrier_semaphore()
    count = 0
    for d in DIRS:
        pl.semaphore_signal(barrier, inc=1, device_id=neighbour(d), device_id_type=MESH)
        count += 1
    for hop in hops[0] + hops[1]:
        pl.semaphore_signal(barrier, inc=1, device_id=peer(hop), device_id_type=MESH)
        count += 1

    row = lax.broadcasted_iota(jnp.int32, (ROWS, lanes), 0)
    lane = lax.broadcasted_iota(jnp.int32, (ROWS, lanes), 1)
    zero = jnp.zeros((ROWS, lanes), f32)

    def load_own(x, carry):
        for y in range(by):
            filled = jnp.zeros((ROWS, lanes), jnp.int32)
            for z in range(bz):
                filled = jnp.where(row == z + 1, counts[x, y, z], filled)
            parts = [offsets[0, x, y], offsets[1, x, y], offsets[2, x, y], mass[x, y], heat[x, y]]
            for k, part in enumerate(parts):
                tile = padded(part)
                if k == 3:
                    tile = jnp.where(lane < filled, tile, 0.0)
                f_own[k, x, y] = tile
                f_all[k, x + 1, y + 1, 1 : bz + 1] = tile[1 : bz + 1]
        return carry

    lax.fori_loop(0, bx, load_own, 0)

    def piece(d):
        src, dst = [], []
        for k in range(3):
            n, base = block[k], 1 if k == 2 else 0
            if d[k] == 0:
                src.append(pl.ds(base, n))
                dst.append(pl.ds(1, n))
            elif d[k] == 1:
                src.append(pl.ds(base + n - 1, 1))
                dst.append(pl.ds(0, 1))
            else:
                src.append(pl.ds(base, 1))
                dst.append(pl.ds(n + 1, 1))
        return tuple(src), tuple(dst)

    def halo_copies(src_ref, lead_src, dst_ref, lead_dst, ssem, rsem):
        copies = []
        for i, d in enumerate(DIRS):
            src, dst = piece(d)
            copies.append(
                pltpu.make_async_remote_copy(
                    src_ref=src_ref.at[(lead_src,) + src],
                    dst_ref=dst_ref.at[(lead_dst,) + dst],
                    send_sem=ssem.at[i],
                    recv_sem=rsem.at[i],
                    device_id=neighbour(d),
                    device_id_type=MESH,
                )
            )
        return copies

    def max_copies(phase):
        begin = phase * len(hops[0])
        return [
            pltpu.make_async_remote_copy(
                src_ref=mx.at[phase],
                dst_ref=mx_parts.at[begin + i],
                send_sem=msend.at[begin + i],
                recv_sem=mrecv.at[begin + i],
                device_id=peer(hop),
                device_id_type=MESH,
            )
            for i, hop in enumerate(hops[phase])
        ]

    def max_result(phase):
        begin = phase * len(hops[0])
        total = mx[phase]
        for i in range(len(hops[phase])):
            total = jnp.maximum(total, mx_parts[begin + i])
        return total

    fields = pl.ds(0, f_own.shape[0])
    first_halo = halo_copies(f_own, fields, f_all, fields, fsend, frecv)

    def greet():
        pl.semaphore_wait(barrier, count)
        for c in first_halo:
            c.start()

    def halo(step):
        return halo_copies(u_own, step, u_all, step, usend.at[step], urecv.at[step])

    sides = (bx + 2) * (by + 2)
    body = functools.partial(
        work, block, lanes, f_own, f_all, u_own, u_all, mx, out, counts, greet, first_halo, halo, max_copies, max_result
    )
    tiles = 22 * ROWS
    group = max((3 * by - 2) * 4, (3 * by - 2) * 2 + 12, 36)
    pl.run_scoped(
        body,
        pltpu.VMEM((bx * by * bz, 27, lanes, lanes), bf16),
        pltpu.VMEM((sides, lanes, tiles), bf16),
        pltpu.VMEM((bx * by, bz // 2, 3, tiles, 2 * lanes), bf16),
        pltpu.VMEM((group, lanes, 2 * lanes), bf16),
        pltpu.VMEM((group, lanes, 2 * lanes), bf16),
        pltpu.VMEM((sides, 3, 4 * ROWS, lanes), bf16),
        pltpu.VMEM((sides, 3, 2 * ROWS, lanes), bf16),
        pltpu.VMEM((sides, 2, ROWS, lanes), f32),
        pltpu.VMEM((bx * by, ROWS, lanes), f32),
        pltpu.VMEM((bx * by, 2, ROWS, lanes), f32),
    )


def work(block, lanes, f_own, f_all, u_own, u_all, mx, out, counts, greet, first_halo, halo, max_copies, max_result,
         k_all, bt, at, buf_a, buf_b, w0_all, w_all, vol, acc, sums):
    bx, by, bz = block
    nx, ny = bx + 2, by + 2
    row = lax.broadcasted_iota(jnp.int32, (ROWS, lanes), 0)
    inside = (row >= 1) & (row <= bz)
    known = row <= bz + 1
    last = ROWS - 1

    def start(copies):
        for c in copies:
            c.start()

    def wait(copies):
        for c in copies:
            c.wait()

    def nearest_first(copies):
        return [copies[i] for i in sorted(range(len(DIRS)), key=lambda i: sum(map(abs, DIRS[i])))]

    def centred(px, py, pz, x, y):
        cx = jnp.asarray(x, jnp.int32).astype(f32) - (0.5 * (bx + 1) + 0.5)
        cy = jnp.asarray(y, jnp.int32).astype(f32) - (0.5 * (by + 1) + 0.5)
        cz = row.astype(f32) - (0.5 * (bz + 1) + 0.5)
        px, py, pz = px + cx, py + cy, pz + cz
        return (px, py, pz), px * px + py * py + pz * pz

    def source(col, x, y, tile_of):
        pos, norm = centred(tile_of(0), tile_of(1), tile_of(2), x, y)
        parts = []
        for p in pos:
            hi, mid, lo = split3(p)
            parts += [hi, mid, hi, mid, lo, hi]
        parts += [jnp.where(row == last, 1.0, part) for part in split3(norm)]
        parts.append(jnp.zeros((ROWS, lanes), f32))
        stack = jnp.concatenate(parts, axis=0).astype(bf16)
        bt[col] = stack.T

    def own_sources(x, carry):
        for y in range(by):
            source((x + 1) * ny + y + 1, x + 1, y + 1, lambda k, y=y: f_own[k, x, y])
        return carry

    lax.fori_loop(0, bx, own_sources, 0)

    def targets(x, carry):
        for y in range(by):
            pos, norm = centred(f_own[0, x, y], f_own[1, x, y], f_own[2, x, y], x + 1, y + 1)
            coefs = [split3(-2.0 * p) for p in pos]
            norms = split3(norm)
            moved = [[[pltpu.roll(part, ez % ROWS, 0) if ez else part for part in c] for c in coefs] for ez in (-1, 0, 1)]
            for zp in range(bz // 2):
                for ez in (-1, 0, 1):
                    halves = []
                    for t in (2 * zp + 1, 2 * zp + 2):
                        here = row == t + ez
                        parts = []
                        for c in moved[ez + 1]:
                            hi, mid, lo = [jnp.where(here, part, 0.0) for part in c]
                            parts += [hi, hi, mid, mid, hi, lo]
                        for part in norms:
                            at_last = pltpu.roll(part, last - t, 0)
                            parts.append(jnp.where(here, 1.0, jnp.where(row == last, at_last, 0.0)))
                        parts.append(jnp.zeros((ROWS, lanes), f32))
                        halves.append(jnp.concatenate(parts, axis=0).astype(bf16))
                    at[x * by + y, zp, ez + 1] = jnp.concatenate(halves, axis=1)
        return carry

    lax.fori_loop(0, bx, targets, 0)
    greet()

    def unit(x, y, cx, cy, zp, ez):
        return dict(t=x * by + y, c=(cx + 1) * ny + cy + 1, zp=zp, ez=ez, slot=((cx - x + 1) * 3 + cy - y + 1) * 3 + ez + 1)

    def gemm(buf, units):
        for i, u in enumerate(units):
            dist_sq = jnp.dot(bt[u["c"]], at[u["t"], u["zp"], u["ez"] + 1], preferred_element_type=f32)
            buf[i] = jnp.maximum(dist_sq.astype(bf16), jnp.array(1e-12, bf16))

    def spread(buf, units):
        for i, u in enumerate(units):
            for half in range(2):
                dist_sq = buf[i, :, half * lanes : (half + 1) * lanes]
                near = jnp.maximum(1.0 - dist_sq * lax.rsqrt(dist_sq), jnp.zeros((), bf16))
                k_all[u["t"] * bz + 2 * u["zp"] + half, u["slot"]] = near * near * near

    def run(now, other, groups, units):
        def step(i, carry):
            gemm(other, units(2 * i + 1))
            spread(now, units(2 * i))
            gemm(now, units(2 * i + 2))
            spread(other, units(2 * i + 1))
            return carry

        lax.fori_loop(0, (groups - 1) // 2, step, 0)
        if groups % 2 == 0:
            gemm(other, units(groups - 1))
            spread(now, units(groups - 2))
            now, other = other, now
        return now, other

    y_pairs = [(y, cy) for y in range(by) for cy in (y - 1, y, y + 1) if 0 <= cy < by]
    y_rims = [(0, -1), (by - 1, by)]
    n_pairs = 3 * bx - 2

    def x_pair(k):
        x = (k + 1) // 3
        return x, k - 2 * x

    def own_units(k):
        x, cx = x_pair(k)
        return [unit(x, y, cx, cy, zp, ez - zp) for zp in (0, 1) for y, cy in y_pairs for ez in (0, 1)]

    def rim_units(k):
        x, cx = x_pair(k)
        return [unit(x, y, cx, cy, zp, 2 * zp - 1) for zp in (0, 1) for y, cy in y_pairs] + [
            unit(x, y, cx, cy, zp, ez) for zp in (0, 1) for y, cy in y_rims for ez in (-1, 0, 1)
        ]

    def far_units(y):
        return [
            unit(x, y, cx, y + ey, zp, ez)
            for x, cx in ((0, -1), (bx - 1, bx))
            for zp in (0, 1)
            for ey in (-1, 0, 1)
            for ez in (-1, 0, 1)
        ]

    gemm(buf_a, own_units(0))
    now, other = run(buf_a, buf_b, n_pairs, own_units)
    wait(first_halo)

    def all_sources(x, carry):
        for y in range(ny):
            source(x * ny + y, x, y, lambda k, y=y: jnp.where(known, f_all[k, x, y], 0.0))
        return carry

    lax.fori_loop(0, nx, all_sources, 0)

    def shifted(ref, col, pairs):
        for ez in (-1, 0, 1):
            his, los = [], []
            for first, second in pairs:
                both = jnp.where(
                    row < bz, pltpu.roll(first, (-1 - ez) % ROWS, 0), pltpu.roll(second, (bz - 1 - ez) % ROWS, 0)
                )
                hi, lo = split2(both)
                his.append(hi)
                los.append(lo)
            ref[col, ez + 1] = jnp.concatenate(his + los, axis=0).astype(bf16)

    def apart(tile):
        return pltpu.roll(tile, 1, 0), pltpu.roll(tile, (1 - bz) % ROWS, 0)

    def weigh_first(x, carry):
        for y in range(ny):
            col = x * ny + y
            v, u = f_all[3, x, y], f_all[HEAT, x, y]
            vc = v * (u * u * jnp.sqrt(u))
            vol[col, 0] = v
            vol[col, 1] = vc
            shifted(w0_all, col, [(v, vc), (v * u, vc * u)])
        return carry

    lax.fori_loop(0, nx, weigh_first, 0)
    gemm(other, rim_units(0))
    spread(now, own_units(n_pairs - 1))
    now, other = run(other, now, n_pairs, rim_units)
    gemm(other, far_units(0))
    spread(now, rim_units(n_pairs - 1))
    now, other = run(other, now, by, far_units)
    spread(now, far_units(by - 1))

    same = lax.broadcasted_iota(jnp.int32, (lanes, lanes), 0) == lax.broadcasted_iota(jnp.int32, (lanes, lanes), 1)
    same = same.astype(f32).astype(bf16)

    def itself(t, carry):
        for z in range(bz):
            k_all[t * bz + z, 13] = jnp.maximum(k_all[t * bz + z, 13], same)
        return carry

    lax.fori_loop(0, bx * by, itself, 0)

    def reduce(w_ref, kinds, x, y, lists):
        total = jnp.zeros((kinds * ROWS, lanes), f32)
        wide = lax.broadcasted_iota(jnp.int32, (kinds * ROWS, lanes), 0) % bz
        for z in range(bz):
            items = [(cx, cy, ez) for cx, cy, ez in lists[z]]
            if not items:
                continue
            w = jnp.concatenate([w_ref[(cx + 1) * ny + cy + 1, ez + 1] for cx, cy, ez in items], axis=1)
            k = jnp.concatenate(
                [k_all[(x * by + y) * bz + z, ((cx - x + 1) * 3 + cy - y + 1) * 3 + ez + 1] for cx, cy, ez in items], axis=0
            )
            o = jnp.dot(w, k, preferred_element_type=f32)
            o = o[: kinds * ROWS] + o[kinds * ROWS :]
            total = jnp.where(wide == z, o, total)
        return total

    def flow_of(s_vu, s_vcu, s_v, s_vc, u, c):
        return c * (s_vu - u * s_v) + (s_vcu - u * s_vc)

    def heat_power(u):
        return u * u * jnp.sqrt(u)

    def emit(step, x, y, flow):
        u_own[step, x, y] = flow
        u_all[step, x + 1, y + 1, 1 : bz + 1] = flow[1 : bz + 1]

    every = [[(ex, ey, ez) for ex in (-1, 0, 1) for ey in (-1, 0, 1) for ez in (-1, 0, 1)] for z in range(bz)]

    def apply_first(x, largest):
        for y in range(by):
            lists = [[(x + ex, y + ey, ez) for ex, ey, ez in every[z]] for z in range(bz)]
            o = reduce(w0_all, 2, x, y, lists)
            s_v, s_vc = apart(o[:ROWS])
            s_vu, s_vcu = apart(o[ROWS:])
            u = f_own[HEAT, x, y]
            c = heat_power(u)
            sums[x * by + y, 0] = s_v
            sums[x * by + y, 1] = s_vc
            emit(0, x, y, jnp.where(inside, flow_of(s_vu, s_vcu, s_v, s_vc, u, c), 0.0))
            rows = c * s_v + s_vc
            lane = lax.broadcasted_iota(jnp.int32, (ROWS, lanes), 1)
            filled = jnp.zeros((ROWS, lanes), jnp.int32)
            for z in range(bz):
                filled = jnp.where(row == z + 1, counts[x, y, z], filled)
            largest = jnp.maximum(largest, jnp.where(inside & (lane < filled), rows, 0.0))
        return largest

    largest = jnp.zeros((ROWS, lanes), f32)
    for x in range(bx):
        largest = apply_first(x, largest)
    mx[0] = largest
    halo1 = halo(0)
    max0 = max_copies(0)
    start(nearest_first(halo1))
    start(max0)

    def weigh(step, x, y, u):
        col = (x + 1) * ny + y + 1
        shifted(w_all, col, [(vol[col, 0] * u, vol[col, 1] * u)])

    own_cols = [(x, y) for x in range(bx) for y in range(by)]
    face_cols = [(x, y) for x in (-1, bx) for y in range(by)] + [(x, y) for x in range(bx) for y in (-1, by)]
    edge_cols = [(x, y) for x in (-1, bx) for y in (-1, by)]

    def outside(x, y, z):
        return sum(not 0 <= i < n for i, n in zip((x, y, z), block))

    def blocks(x, y, wanted):
        return [
            [(x + ex, y + ey, ez) for ex, ey, ez in every[z] if outside(x + ex, y + ey, z + ez) in wanted] for z in range(bz)
        ]

    def apply_own(step):
        for x, y in own_cols:
            weigh(step, x, y, u_own[step, x, y])
        for x, y in own_cols:
            acc[x * by + y] = reduce(w_all, 1, x, y, blocks(x, y, (0,)))

    def apply_faces(step, copies):
        wait([c for c, d in zip(copies, DIRS) if sum(map(abs, d)) == 1])
        for x, y in own_cols:
            weigh(step, x, y, u_all[step, x + 1, y + 1])
        for x, y in face_cols:
            weigh(step, x, y, padded(u_all[step, x + 1, y + 1, 1 : bz + 1]))
        for x, y in own_cols:
            acc[x * by + y] += reduce(w_all, 1, x, y, blocks(x, y, (1,)))

    def apply_rest(step, copies, emit_flow):
        wait([c for c, d in zip(copies, DIRS) if sum(map(abs, d)) > 1])
        for x, y in face_cols + edge_cols:
            weigh(step, x, y, u_all[step, x + 1, y + 1])
        for x, y in own_cols:
            t = x * by + y
            s_vu, s_vcu = apart(acc[t] + reduce(w_all, 1, x, y, blocks(x, y, (2, 3))))
            u = u_own[step, x, y]
            emit_flow(x, y, flow_of(s_vu, s_vcu, sums[t, 0], sums[t, 1], u, heat_power(f_own[HEAT, x, y])))

    apply_own(0)
    apply_faces(0, halo1)
    apply_rest(0, halo1, lambda x, y, flow: emit(1, x, y, jnp.where(inside, flow, 0.0)))
    halo2 = halo(1)
    start(nearest_first(halo2))
    wait(max0)
    mx[1] = max_result(0)
    max1 = max_copies(1)
    start(max1)
    apply_own(1)
    apply_faces(1, halo2)
    wait(max1)
    top = jnp.max(jnp.max(max_result(1), axis=1, keepdims=True), axis=0, keepdims=True)
    step = 2.0 / top

    def finish(x, y, f2):
        f0, f1 = u_own[0, x, y], u_own[1, x, y]
        d_first = 2.0 / 15.0 * step * f0
        l_first = f0 + 2.0 / 15.0 * step * f1
        l_l_first = f1 + 2.0 / 15.0 * step * f2
        d_second = 1.5 * d_first + 0.6 * step * l_first - 0.4 * step * f0
        l_second = 1.5 * l_first - 0.5 * f0 + 0.6 * step * l_l_first - 0.4 * step * f1
        rise = 25.0 / 12.0 * d_second - 5.0 / 6.0 * d_first + 5.0 / 6.0 * step * l_second - 5.0 / 9.0 * step * f0
        out[x, y] = rise[1 : bz + 1]

    apply_rest(1, halo2, finish)


def local(relative_placements, mass_per_density, opening_heat_level, bin_fill_counts):
    lanes = opening_heat_level.shape[-1]
    block = opening_heat_level.shape[:3]
    dims = tuple(lax.axis_size(a) for a in AXES)
    bx, by, bz = block
    assert bz == 4
    vmem = pl.BlockSpec(memory_space=pltpu.VMEM)
    dma = pltpu.SemaphoreType.DMA
    n_dirs = len(DIRS)
    n_peers = dims[0] - 1 + dims[1] * dims[2] - 1
    rise = pl.pallas_call(
        functools.partial(kernel, dims, block),
        out_shape=jax.ShapeDtypeStruct(block + (lanes,), f32),
        in_specs=[pl.BlockSpec(memory_space=pltpu.SMEM), vmem, vmem, vmem],
        out_specs=vmem,
        scratch_shapes=[
            pltpu.VMEM((HEAT + 1, bx, by, ROWS, lanes), f32),
            pltpu.VMEM((HEAT + 1, bx + 2, by + 2, ROWS, lanes), f32),
            pltpu.VMEM((2, bx, by, ROWS, lanes), f32),
            pltpu.VMEM((2, bx + 2, by + 2, ROWS, lanes), f32),
            pltpu.VMEM((2, ROWS, lanes), f32),
            pltpu.VMEM((n_peers, ROWS, lanes), f32),
            dma((n_dirs,)),
            dma((n_dirs,)),
            dma((2, n_dirs)),
            dma((2, n_dirs)),
            dma((n_peers,)),
            dma((n_peers,)),
        ],
        compiler_params=pltpu.CompilerParams(
            collective_id=0, has_side_effects=True, vmem_limit_bytes=60 * 1024 * 1024
        ),
    )(bin_fill_counts, relative_placements, mass_per_density, opening_heat_level)
    return opening_heat_level + rise


def solution(mesh):
    in_specs = (
        P(None, "gx", "gy", "gz", None),
        P("gx", "gy", "gz", None),
        P("gx", "gy", "gz", None),
        P("gx", "gy", "gz"),
    )
    out_specs = P("gx", "gy", "gz", None)
    return jax.shard_map(local, mesh=mesh, in_specs=in_specs, out_specs=out_specs, check_vma=False)
```
